256 devices in a mesh: groups: 2 (over y), expert: 4 (over x), etp: 32 (over z, core).
Axes of the slice: x: 4, y: 2, z: 16, core: 2. Of those that a mesh axis runs over, the one named last changes fastest.
The devices are a block of a 4x16x16 slice.
Arguments:
- tokens: bfloat16 [1024, 4096], P(('groups', 'expert'), 'etp'), parts along dimension 0, may hold values from -6 to 6
- route_ids: int32 [1024, 2], P(('groups', 'expert')), parts along dimension 0, may hold values from 0 to 3, all different within a row; in each aligned block of 128 rows (0 to 127, 128 to 255, ...) at most 96 rows name the same one
- gate_weights: float32 [1024, 2], P(('groups', 'expert')), parts along dimension 0, may hold values from 0.2 to 1
- w_gate: bfloat16 [4, 4096, 14336], P('expert', None, 'etp'), may hold values from -0.09375 to 0.09375
- w_up: bfloat16 [4, 4096, 14336], P('expert', None, 'etp'), may hold values from -0.09375 to 0.09375
- w_down: bfloat16 [4, 14336, 4096], P('expert', 'etp'), may hold values from -0.09375 to 0.09375
Outputs:
- mixed: bfloat16 [1024, 4096], P(('groups', 'expert'), 'etp'), parts along dimension 0
The draws below stay inside these ranges and needn't reach their ends.
There are 2 independent parts, one for each index of `groups`. The reference program is written for one: setup_inputs(seed, part) draws one part's arguments, and reference() takes and returns one part's arrays. A program takes and returns all parts, laid end to end along the dimension named above; an argument that names none is the same for every part. Nothing has to cross between parts.
Inputs may be any that keep to these rules, and one draw needn't show every extreme that they name: `route_ids`: each row names two different experts. In the rows of one index of expert (128 aligned rows), no expert is named by more than 96 rows, a bound that some block reaches.
All inputs are finite; a program needn't handle non-finite values.
Results may differ from the reference program's by a relative error of at most 0.024.
Values may be sent and summed in bfloat16 or wider, within the bound.
No kernel may reach another device: no remote copies, remote signals or barrier semaphores. Data moves between devices by JAX's collectives and lax.ppermute only.
A program may use at most 64 MiB of HBM per device.

```python
import math
import jax
import jax.numpy as jnp
import numpy as np
from jax import lax

D = 4096
FF = 14336
TOK_DEV = 128
CAP = 96
EXPERTS = 4
TOKENS = 512
N_EXPERT = 4
N_ETP = 32


def spiked(drawn, key, source, target, parts, factor):
    owner, partner = [(jnp.arange(drawn.shape[dim]) // (drawn.shape[dim] // parts)).reshape([-1 if axis == dim else 1 for axis in range(drawn.ndim)]) for dim in (source, target)]
    chosen = jax.random.permutation(key, parts)[partner]
    strong = (owner == chosen) | (owner == (partner + parts // 2) % parts)
    return jnp.where(strong, factor * drawn, drawn)


def shard_levels(key, dims, pieces, smallest, largest):
    level = 1.0
    for dim, blocks in pieces:
        heights = jax.random.uniform(jax.random.fold_in(jax.random.fold_in(key, 6), dim), (blocks,), jnp.float32, smallest / len(pieces), largest / len(pieces))
        level = level * jnp.repeat(jnp.exp(heights), dims[dim] // blocks).reshape((-1,) + (1,) * (len(dims) - 1 - dim))
    return level


def shared_out(rng, own, number, rows, amount, top, limit, skew):
    ranking = jax.random.permutation(rng, amount)
    packed, ordinary = shares(amount, rows * top, limit, skew, True), shares(amount, rows * top, limit, skew, False)
    places = jnp.arange(amount)

    def named(sizes, offset_by):
        used = int((sizes > 0).sum())
        fixed = max(1, used // 4)
        passed = fixed + (places - fixed + offset_by * (used - fixed)) % max(1, amount - fixed)
        return jnp.zeros((amount,), jnp.int32).at[ranking[jnp.where(places < fixed, places, passed)]].set(jnp.asarray(sizes, jnp.int32))

    sizes = jnp.where(number % 4 == 0, named(packed, number // 4), named(ordinary, number - number // 4 - 1))
    mixed = jax.random.permutation(jax.random.fold_in(own, 3), amount)
    source_of, taker = mixed[0:amount // 2 * 2:2], mixed[1:amount // 2 * 2:2]
    room = jnp.minimum(sizes[source_of] - 1, limit - sizes[taker]) // 2
    room = jnp.where((source_of == ranking[0]) | (taker == ranking[0]) | (sizes[taker] == 0), 0, jnp.maximum(room, 0))
    passed = jax.random.randint(jax.random.fold_in(own, 4), (amount // 2,), 0, 1 << 20) % (room + 1)
    sizes = sizes.at[source_of].add(-passed).at[taker].add(passed)
    members = jnp.searchsorted(jnp.cumsum(sizes), jnp.arange(rows * top), side="right").astype(jnp.int32)
    table = members.reshape(top, rows).T
    table = table[jax.random.permutation(jax.random.fold_in(own, 1), rows)]
    offset_by = jax.random.randint(jax.random.fold_in(own, 2), (rows, 1), 0, top)
    return jnp.take_along_axis(table, (jnp.arange(top)[None, :] + offset_by) % top, axis=1)


def shares(number_of, total, reach, skew, full):
    portions = [(1 << 20) // math.isqrt(rank ** skew) + 1 for rank in range(1, number_of + 1)]
    largest = reach if full else min(reach, max(-(-total // number_of), total * portions[0] // sum(portions)))
    least = 1 if total - largest >= number_of - 1 else 0
    counts, spare = [largest] + [least] * (number_of - 1), total - largest - least * (number_of - 1)
    while spare > 0:
        movable = [i for i in range(1, number_of) if counts[i] < largest] or [i for i in range(1, number_of) if counts[i] < reach]
        pool, budget = sum([portions[i] for i in movable]), spare
        for i in movable:
            more = min(reach - counts[i], max(1, budget * portions[i] // pool), spare)
            counts[i] = counts[i] + more
            spare = spare - more
    return np.array(counts)


def noise(rng, dims, spread, limit, cuts=(), held_as=jnp.bfloat16):
    drawn = jax.random.normal(rng, dims, jnp.float32) * spread
    if len(cuts) > 0:
        drawn = shard_levels(rng, dims, cuts, -0.22, 0.18) * drawn
    return jnp.clip(drawn, min=-limit, max=limit).astype(held_as)


def bell_draw_with(key, extent, width, limit, shards, heavy, kind=jnp.bfloat16):
    result = width * jax.random.normal(key, extent, jnp.float32)
    if shards:
        result = result * shard_levels(key, extent, shards, -0.22, 0.18)
    return jnp.clip(spiked(result, jax.random.fold_in(key, 3), *heavy), -limit, limit).astype(kind)


def setup_inputs(seed: int = 0, part: int = 0) -> dict:
    streams_of = jax.random.split(jax.random.key(seed), 7)
    part_splits = jax.random.split(jax.random.fold_in(streams_of[6], part), 7)
    tokens = noise(part_splits[0], (TOKENS, D), 1.0, 6.0, ((0, 4), (1, 32)))
    route_ids_keys = jax.random.split(jax.random.fold_in(part_splits[1], 1), TOKENS // TOK_DEV)
    route_ids_turns = jax.random.permutation(jax.random.fold_in(part_splits[1], 3), TOKENS // TOK_DEV)
    route_ids = jax.vmap(lambda own, number: shared_out(jax.random.fold_in(part_splits[1], 2), own, number, TOK_DEV, EXPERTS, 2, CAP, 1))(route_ids_keys, route_ids_turns).reshape((TOKENS, 2))
    gate_weights = jnp.clip(0.2 + 0.8 * jax.random.uniform(part_splits[2], (TOKENS, 2), jnp.float32) ** shard_levels(part_splits[2], (TOKENS, 2), ((0, 4),), -0.2, 0.2), 0.2, 1.0)
    w_gate = noise(streams_of[3], (EXPERTS, D, FF), D ** -0.5, 0.09375, ((0, 4), (2, 32)))
    w_up = noise(streams_of[4], (EXPERTS, D, FF), D ** -0.5, 0.09375, ((0, 4), (2, 32)))
    w_down = bell_draw_with(streams_of[5], (EXPERTS, FF, D), FF ** -0.5, 0.09375, ((0, 4), (1, 32)), (1, 2, 32, 2.75))
    return {"tokens": tokens, "route_ids": route_ids, "gate_weights": gate_weights, "w_gate": w_gate, "w_up": w_up, "w_down": w_down}


def down_sum(hidden_wide, down_wide):
    group = FF // N_ETP
    rows = hidden_wide.shape[0]

    def add_group(index, total):
        start = (index * group).astype(jnp.int32)
        hidden_part = lax.dynamic_slice_in_dim(hidden_wide, start, group, 1)
        down_part = lax.dynamic_slice_in_dim(down_wide, start, group, 0)
        partial_value = jnp.dot(hidden_part, down_part, precision=lax.Precision.HIGHEST).astype(jnp.bfloat16)
        return total + partial_value.astype(jnp.float32)

    return lax.fori_loop(0, N_ETP, add_group, jnp.zeros((rows, D), jnp.float32))


def reference(tokens, route_ids, gate_weights, w_gate, w_up, w_down):
    slot_total = N_EXPERT * CAP
    summed = jnp.zeros((TOKENS, D), jnp.float32)
    token_block = (jnp.arange(TOKENS, dtype=jnp.int32) // TOK_DEV).astype(jnp.int32)
    for expert_number in range(EXPERTS):
        hit_mask = route_ids == expert_number
        routed = jnp.any(hit_mask, axis=1).astype(jnp.int32)
        weighting = jnp.sum(jnp.where(hit_mask, gate_weights, 0.0), axis=1)
        slot_index = (jnp.cumsum(routed.reshape(N_EXPERT, TOK_DEV), axis=1) - 1).reshape(TOKENS).astype(jnp.int32)
        target_row = jnp.where(routed == 1, token_block * CAP + slot_index, slot_total).astype(jnp.int32)
        buffer = jnp.zeros((slot_total, D), jnp.bfloat16).at[target_row].set(tokens, mode="drop")
        buffer_wide = buffer.astype(jnp.float32)
        gate_sum = jnp.dot(buffer_wide, w_gate[expert_number].astype(jnp.float32), precision=lax.Precision.HIGHEST)
        up_sum = jnp.dot(buffer_wide, w_up[expert_number].astype(jnp.float32), precision=lax.Precision.HIGHEST)
        hidden = (jax.nn.silu(gate_sum) * up_sum).astype(jnp.bfloat16)
        expert_out = down_sum(hidden.astype(jnp.float32), w_down[expert_number].astype(jnp.float32)).astype(jnp.bfloat16)
        picked = expert_out[jnp.minimum(target_row, slot_total - 1)]
        summed = summed + weighting[:, None] * picked.astype(jnp.float32)
    return summed.astype(jnp.bfloat16)
```

```python
import functools

import jax
import jax.numpy as jnp
from jax import lax
from jax.experimental import pallas as pl
from jax.experimental.pallas import tpu as pltpu
from jax.sharding import Mesh
from jax.sharding import PartitionSpec as P

CAP = 96
CORES = 2
ETP = ("etp_0", "etp_1")
LANES = 128
CHUNKS = 4

VMEM = pl.BlockSpec(memory_space=pltpu.VMEM)
SMEM = pl.BlockSpec(memory_space=pltpu.SMEM)
ANY = pl.BlockSpec(memory_space=pl.ANY)


def dot32(a, b):
    return jnp.dot(a, b, preferred_element_type=jnp.float32)


def columns_of(ref, start, count):
    groups, _, rows, lanes = ref.shape
    parts = [ref[:, z].reshape(groups * rows, lanes) for z in range(start, start + count)]
    return jnp.concatenate(parts, axis=1)


def dispatch_body(table_ref, tokens_ref, out_ref):
    experts, chips, cap, lanes = out_ref.shape
    table = table_ref[...]
    for z in range(0, chips, 2):
        pair = jnp.concatenate([tokens_ref[z], tokens_ref[z + 1]], axis=1)
        rows = dot32(table, pair).astype(out_ref.dtype)
        for k in range(2):
            out_ref[:, z + k] = rows[:, k * lanes : (k + 1) * lanes].reshape(experts, cap, lanes)


def weight_copies(core, w_refs, bufs, sems):
    chips = bufs[0].shape[0]
    step = chips // CHUNKS
    return [
        [
            pltpu.make_async_copy(
                w.at[pl.ds(k * step, step), core], buf.at[pl.ds(k * step, step)], sems.at[i, k]
            )
            for i, (w, buf) in enumerate(zip(w_refs, bufs))
        ]
        for k in range(CHUNKS)
    ]


def up_partial(copies, x_ref, bufs, emit):
    chips, lanes, width = bufs[0].shape
    step = chips // CHUNKS
    for k in range(CHUNKS):
        for copy in copies[k]:
            copy.wait()
        x = columns_of(x_ref, k * step, step)
        emit(k, [dot32(x, buf[k * step : (k + 1) * step].reshape(step * lanes, width)) for buf in bufs])


def first_half_body(core_ref, x_ref, wg_ref, wu_ref, gate_ref, up_ref, g_buf, u_buf, sems):
    copies = weight_copies(core_ref[0], (wg_ref, wu_ref), (g_buf, u_buf), sems)
    for chunk in copies:
        for copy in chunk:
            copy.start()

    def emit(k, sums):
        for ref, value in zip((gate_ref, up_ref), sums):
            ref[...] = value if k == 0 else ref[...] + value

    up_partial(copies, x_ref, (g_buf, u_buf), emit)


def down_copies(core, wd_ref, d_buf, sem):
    chips = d_buf.shape[1] // LANES
    return [
        pltpu.make_async_copy(
            wd_ref.at[:, pl.ds(pl.multiple_of((z * CORES + core) * LANES, LANES), LANES)],
            d_buf.at[:, pl.ds(z * LANES, LANES)],
            sem.at[z],
        )
        for z in range(chips)
    ]


def down_into(copies, hidden, d_buf, out_ref):
    blocks, chips, cap, lanes = out_ref.shape
    step = chips // CHUNKS
    for k in range(CHUNKS):
        for copy in copies[k * step : (k + 1) * step]:
            copy.wait()
        part = dot32(hidden, d_buf[:, k * step * lanes : (k + 1) * step * lanes]).astype(out_ref.dtype)
        for z in range(step):
            out_ref[:, k * step + z] = part[:, z * lanes : (z + 1) * lanes].reshape(blocks, cap, lanes)


def second_half_body(
    core_ref, x_ref, gate_ref, up_ref, wg_ref, wu_ref, wd_ref, hidden_ref, out_ref, g_buf, u_buf, d_buf, g_acc, u_acc, sems, d_sem
):
    other = 1 - core_ref[0]
    copies = weight_copies(other, (wg_ref, wu_ref), (g_buf, u_buf), sems)
    downs = down_copies(other, wd_ref, d_buf, d_sem)
    for chunk in copies:
        for copy in chunk:
            copy.start()
    for copy in downs:
        copy.start()

    def emit(k, sums):
        for ref, base, value in zip((g_acc, u_acc), (gate_ref, up_ref), sums):
            ref[...] = (base if k == 0 else ref)[...] + value

    up_partial(copies, x_ref, (g_buf, u_buf), emit)
    gate = g_acc[...]
    hidden = (gate / (1.0 + jnp.exp(-gate)) * u_acc[...]).astype(jnp.bfloat16)
    hidden_ref[...] = hidden
    down_into(downs, hidden, d_buf, out_ref)


def own_down_body(core_ref, hidden_ref, wd_ref, out_ref, d_buf, d_sem):
    downs = down_copies(core_ref[0], wd_ref, d_buf, d_sem)
    for copy in downs:
        copy.start()
    down_into(downs, hidden_ref[...], d_buf, out_ref)


def combine_body(table_ref, results_ref, out_ref):
    chips, _, lanes = out_ref.shape
    table = table_ref[...]
    for z in range(0, chips, 2):
        rows = dot32(table, columns_of(results_ref, z, 2)).astype(out_ref.dtype)
        for k in range(2):
            out_ref[z + k] = rows[:, k * lanes : (k + 1) * lanes]


def call(body, out_shape, in_specs, scratch=(), flops=0):
    outs = jax.tree.map(lambda _: VMEM, out_shape)
    return pl.pallas_call(
        body,
        out_shape=out_shape,
        in_specs=list(in_specs),
        out_specs=outs,
        scratch_shapes=list(scratch),
        cost_estimate=pl.CostEstimate(flops=flops, transcendentals=0, bytes_accessed=flops // 400),
        compiler_params=pltpu.CompilerParams(vmem_limit_bytes=40 * 1024 * 1024),
    )


def shards(tokens, route_ids, gate_weights, w_gate, w_up, w_down):
    experts = lax.axis_size("expert")
    chips = lax.axis_size("etp_0")
    token_count, lanes = tokens.shape
    slots = experts * CAP
    _, width_in, width = w_gate.shape
    bf16, f32 = jnp.bfloat16, jnp.float32
    shape = jax.ShapeDtypeStruct

    expert_iota = lax.broadcasted_iota(jnp.int32, (1, 1, experts), 2)
    hit_mask = route_ids[:, :, None] == expert_iota
    routed = jnp.any(hit_mask, axis=1).astype(jnp.int32)
    weighting = jnp.sum(jnp.where(hit_mask, gate_weights[:, :, None], 0.0), axis=1)
    slot_index = jnp.cumsum(routed, axis=0) - 1
    expert_base = lax.broadcasted_iota(jnp.int32, (1, experts), 1) * CAP
    target_slot = jnp.where(routed == 1, expert_base + slot_index, -1)
    slot_iota = lax.broadcasted_iota(jnp.int32, (1, 1, slots), 2)
    pick_table = target_slot[:, :, None] == slot_iota
    select_table = jnp.any(pick_table, axis=1).astype(bf16).T
    combine_table = jnp.sum(jnp.where(pick_table, weighting[:, :, None], 0.0), axis=1).astype(bf16)

    core = lax.axis_index("etp_1").astype(jnp.int32).reshape(1)
    swap = functools.partial(lax.ppermute, axis_name="etp_1", perm=[(0, 1), (1, 0)])
    exchange = functools.partial(lax.all_to_all, split_axis=0, concat_axis=0, tiled=True)

    gathered = lax.all_gather(tokens, "etp_0", axis=0, tiled=False)
    sent = call(
        dispatch_body, shape((experts, chips, CAP, lanes), bf16), (VMEM, VMEM), flops=2 * slots * token_count * chips * lanes
    )(select_table, gathered)
    own = exchange(sent, "expert")
    other = swap(own)

    gate_rows = w_gate.reshape(chips, CORES, lanes, width)
    up_rows = w_up.reshape(chips, CORES, lanes, width)
    down_rows = w_down[0]
    up_flops = 2 * slots * width * width_in
    w_bufs = [pltpu.VMEM((chips, lanes, width), bf16)] * 2
    w_sems = pltpu.SemaphoreType.DMA((2, CHUNKS))
    d_buf = pltpu.VMEM((width, chips * lanes), bf16)
    d_sem = pltpu.SemaphoreType.DMA((chips,))
    acc = shape((slots, width), f32)
    gate_half, up_half = call(
        first_half_body, (acc, acc), (SMEM, VMEM, ANY, ANY), [*w_bufs, w_sems], flops=up_flops
    )(core, own, gate_rows, up_rows)
    hidden, theirs = call(
        second_half_body,
        (shape((slots, width), bf16), shape((experts, chips, CAP, lanes), bf16)),
        (SMEM, VMEM, VMEM, VMEM, ANY, ANY, ANY),
        [*w_bufs, d_buf, pltpu.VMEM((slots, width), f32), pltpu.VMEM((slots, width), f32), w_sems, d_sem],
        flops=up_flops * 3 // 2,
    )(core, other, gate_half, up_half, gate_rows, up_rows, down_rows)
    arrived = swap(theirs)
    mine = call(
        own_down_body, shape((experts, chips, CAP, lanes), f32), (SMEM, VMEM, ANY), [d_buf, d_sem], flops=up_flops // 2
    )(core, hidden, down_rows)
    chip_sum = (mine + arrived.astype(f32)).astype(bf16)
    results = exchange(chip_sum, "expert")
    blended = call(
        combine_body, shape((chips, token_count, lanes), bf16), (VMEM, VMEM), flops=2 * slots * token_count * chips * lanes
    )(combine_table, results)
    pieces = exchange(blended, "etp_0")
    return pieces.astype(f32).sum(axis=0).astype(bf16)


def solution(mesh):
    groups, experts, etp = (mesh.shape[name] for name in ("groups", "expert", "etp"))
    finer = Mesh(
        mesh.devices.reshape(groups, experts, etp // CORES, CORES),
        ("groups", "expert", "etp_0", "etp_1"),
    )
    placed = (
        P(("groups", "expert"), ETP),
        P(("groups", "expert"), None),
        P(("groups", "expert"), None),
        P("expert", None, ETP),
        P("expert", None, ETP),
        P("expert", ETP, None),
    )
    return jax.shard_map(
        shards, mesh=finer, in_specs=placed, out_specs=P(("groups", "expert"), ETP), check_vma=False
    )
```

```python
import functools

import jax
import jax.numpy as jnp
from jax import lax
from jax.experimental import pallas as pl
from jax.experimental.pallas import tpu as pltpu
from jax.sharding import Mesh
from jax.sharding import PartitionSpec as P

CAP = 96
CORES = 2
ETP = ("etp_0", "etp_1")
LANES = 128
CHUNKS = 4

VMEM = pl.BlockSpec(memory_space=pltpu.VMEM)
SMEM = pl.BlockSpec(memory_space=pltpu.SMEM)


def dot32(a, b):
    return jnp.dot(a, b, preferred_element_type=jnp.float32)


def columns_of(ref, start, count):
    groups, _, rows, lanes = ref.shape
    parts = [ref[:, z].reshape(groups * rows, lanes) for z in range(start, start + count)]
    return jnp.concatenate(parts, axis=1)


def dispatch_body(table_ref, tokens_ref, out_ref):
    experts, chips, cap, lanes = out_ref.shape
    table = table_ref[...]
    for z in range(0, chips, 2):
        pair = jnp.concatenate([tokens_ref[z], tokens_ref[z + 1]], axis=1)
        rows = dot32(table, pair).astype(out_ref.dtype)
        for k in range(2):
            out_ref[:, z + k] = rows[:, k * lanes : (k + 1) * lanes].reshape(experts, cap, lanes)


def core_columns(ref, core, start, count):
    parts = [
        ref[:, pl.ds(pl.multiple_of((z * CORES + core) * LANES, LANES), LANES)] for z in range(start, start + count)
    ]
    return jnp.concatenate(parts, axis=1)


def up_partial(core, x_ref, w_refs):
    chips = x_ref.shape[1]
    step = chips // CHUNKS
    sums = [None] * len(w_refs)
    for k in range(CHUNKS):
        x = columns_of(x_ref, k * step, step)
        for i, w in enumerate(w_refs):
            part = lax.dot_general(
                x, core_columns(w, core, k * step, step), (((1,), (1,)), ((), ())), preferred_element_type=jnp.float32
            )
            sums[i] = part if k == 0 else sums[i] + part
    return sums


def down_into(core, hidden, wd_ref, out_ref):
    blocks, chips, cap, lanes = out_ref.shape
    step = chips // CHUNKS
    for k in range(CHUNKS):
        part = dot32(hidden, core_columns(wd_ref, core, k * step, step)).astype(out_ref.dtype)
        for z in range(step):
            out_ref[:, k * step + z] = part[:, z * lanes : (z + 1) * lanes].reshape(blocks, cap, lanes)


def first_half_body(core_ref, x_ref, wg_ref, wu_ref, gate_ref, up_ref):
    gate_ref[...], up_ref[...] = up_partial(core_ref[0], x_ref, (wg_ref, wu_ref))


def second_half_body(core_ref, x_ref, gate_ref, up_ref, wg_ref, wu_ref, wd_ref, hidden_ref, out_ref):
    other = 1 - core_ref[0]
    gate, up = up_partial(other, x_ref, (wg_ref, wu_ref))
    gate = gate + gate_ref[...]
    up = up + up_ref[...]
    hidden = (gate / (1.0 + jnp.exp(-gate)) * up).astype(jnp.bfloat16)
    hidden_ref[...] = hidden
    down_into(other, hidden, wd_ref, out_ref)


def own_down_body(core_ref, hidden_ref, wd_ref, out_ref):
    down_into(core_ref[0], hidden_ref[...], wd_ref, out_ref)


def combine_body(table_ref, results_ref, out_ref):
    chips, _, lanes = out_ref.shape
    table = table_ref[...]
    for z in range(0, chips, 2):
        rows = dot32(table, columns_of(results_ref, z, 2)).astype(out_ref.dtype)
        for k in range(2):
            out_ref[z + k] = rows[:, k * lanes : (k + 1) * lanes]


def call(body, out_shape, in_specs, flops=0):
    outs = jax.tree.map(lambda _: VMEM, out_shape)
    return pl.pallas_call(
        body,
        out_shape=out_shape,
        in_specs=list(in_specs),
        out_specs=outs,
        cost_estimate=pl.CostEstimate(flops=flops, transcendentals=0, bytes_accessed=flops // 400),
        compiler_params=pltpu.CompilerParams(vmem_limit_bytes=24 * 1024 * 1024),
    )


def shards(tokens, route_ids, gate_weights, w_gate, w_up, w_down):
    experts = lax.axis_size("expert")
    chips = lax.axis_size("etp_0")
    token_count, lanes = tokens.shape
    slots = experts * CAP
    _, width_in, width = w_gate.shape
    bf16, f32 = jnp.bfloat16, jnp.float32
    shape = jax.ShapeDtypeStruct

    expert_iota = lax.broadcasted_iota(jnp.int32, (1, 1, experts), 2)
    hit_mask = route_ids[:, :, None] == expert_iota
    routed = jnp.any(hit_mask, axis=1).astype(jnp.int32)
    weighting = jnp.sum(jnp.where(hit_mask, gate_weights[:, :, None], 0.0), axis=1)
    slot_index = jnp.cumsum(routed, axis=0) - 1
    expert_base = lax.broadcasted_iota(jnp.int32, (1, experts), 1) * CAP
    target_slot = jnp.where(routed == 1, expert_base + slot_index, -1)
    slot_iota = lax.broadcasted_iota(jnp.int32, (1, 1, slots), 2)
    pick_table = target_slot[:, :, None] == slot_iota
    select_table = jnp.any(pick_table, axis=1).astype(bf16).T
    combine_table = jnp.sum(jnp.where(pick_table, weighting[:, :, None], 0.0), axis=1).astype(bf16)

    select_table, combine_table = lax.optimization_barrier((select_table, combine_table))

    core = lax.axis_index("etp_1").astype(jnp.int32).reshape(1)
    swap = functools.partial(lax.ppermute, axis_name="etp_1", perm=[(0, 1), (1, 0)])
    exchange = functools.partial(lax.all_to_all, split_axis=0, concat_axis=0, tiled=True)

    gathered = lax.all_gather(tokens, "etp_0", axis=0, tiled=False)
    sent = call(
        dispatch_body, shape((experts, chips, CAP, lanes), bf16), (VMEM, VMEM), flops=2 * slots * token_count * chips * lanes
    )(select_table, gathered)
    own = exchange(sent, "expert")
    other = swap(own)

    gate_rows = jnp.swapaxes(w_gate[0], 0, 1)
    up_rows = jnp.swapaxes(w_up[0], 0, 1)
    down_rows = w_down[0]
    up_flops = 2 * slots * width * width_in
    acc = shape((slots, width), f32)
    gate_half, up_half = call(first_half_body, (acc, acc), (SMEM, VMEM, VMEM, VMEM), flops=up_flops)(
        core, own, gate_rows, up_rows
    )
    hidden, theirs = call(
        second_half_body,
        (shape((slots, width), bf16), shape((experts, chips, CAP, lanes), bf16)),
        (SMEM, VMEM, VMEM, VMEM, VMEM, VMEM, VMEM),
        flops=up_flops * 3 // 2,
    )(core, other, gate_half, up_half, gate_rows, up_rows, down_rows)
    arrived = swap(theirs)
    mine = call(
        own_down_body, shape((experts, chips, CAP, lanes), f32), (SMEM, VMEM, VMEM), flops=up_flops // 2
    )(core, hidden, down_rows)
    chip_sum = (mine + arrived.astype(f32)).astype(bf16)
    results = exchange(chip_sum, "expert")
    blended = call(
        combine_body, shape((chips, token_count, lanes), bf16), (VMEM, VMEM), flops=2 * slots * token_count * chips * lanes
    )(combine_table, results)
    pieces = exchange(blended, "etp_0")
    return pieces.astype(f32).sum(axis=0).astype(bf16)


def solution(mesh):
    groups, experts, etp = (mesh.shape[name] for name in ("groups", "expert", "etp"))
    finer = Mesh(
        mesh.devices.reshape(groups, experts, etp // CORES, CORES),
        ("groups", "expert", "etp_0", "etp_1"),
    )
    placed = (
        P(("groups", "expert"), ETP),
        P(("groups", "expert"), None),
        P(("groups", "expert"), None),
        P("expert", None, ETP),
        P("expert", None, ETP),
        P("expert", ETP, None),
    )
    return jax.shard_map(
        shards, mesh=finer, in_specs=placed, out_specs=P(("groups", "expert"), ETP), check_vma=False
    )
```

```python
import functools

import jax
import jax.numpy as jnp
from jax import lax
from jax.experimental import pallas as pl
from jax.experimental.pallas import tpu as pltpu
from jax.sharding import Mesh
from jax.sharding import PartitionSpec as P

CAP = 96
CORES = 2
Z = ("z_0", "z_1")
ETP = (*Z, "core")
LANES = 128
CHUNKS = 4
AHEAD = 2
PARITIES = 2

HBM = pl.BlockSpec(memory_space=pltpu.HBM)
VMEM = pl.BlockSpec(memory_space=pltpu.VMEM)
SMEM = pl.BlockSpec(memory_space=pltpu.SMEM)


def dot32(a, b):
    return jnp.dot(a, b, preferred_element_type=jnp.float32)


def columns_of(ref, start, count):
    groups, _, rows, lanes = ref.shape
    parts = [ref[:, z].reshape(groups * rows, lanes) for z in range(start, start + count)]
    return jnp.concatenate(parts, axis=1)


def dispatch_body(table_ref, tokens_ref, out_ref):
    experts, chips, cap, lanes = out_ref.shape
    table = table_ref[...]
    for z in range(0, chips, 2):
        pair = jnp.concatenate([tokens_ref[z], tokens_ref[z + 1]], axis=1)
        rows = dot32(table, pair).astype(out_ref.dtype)
        for k in range(2):
            out_ref[:, z + k] = rows[:, k * lanes : (k + 1) * lanes].reshape(experts, cap, lanes)


def core_copies(w_ref, core, buf, sems, first=0):
    return [
        pltpu.make_async_copy(
            w_ref.at[:, pl.ds(pl.multiple_of(((first + k) * CORES + core) * LANES, LANES), LANES)],
            buf.at[:, pl.ds(k * LANES, LANES)],
            sems.at[k],
        )
        for k in range(buf.shape[1] // LANES)
    ]


def start_all(copies):
    for copy in copies:
        copy.start()


def wait_all(copies):
    for copy in copies:
        if copy is not None:
            copy.wait()


def chunk_of(bufs, k, size):
    for buf in bufs:
        if k * size < buf.shape[1]:
            return buf[:, k * size : (k + 1) * size]
        k -= buf.shape[1] // size


def up_partial(x_ref, weights):
    chips = x_ref.shape[1]
    step = chips // CHUNKS
    sums = [None] * len(weights)
    for k in range(CHUNKS):
        x = columns_of(x_ref, k * step, step)
        for i, (copies, bufs) in enumerate(weights):
            wait_all(copies[k * step : (k + 1) * step])
            part = lax.dot_general(
                x, chunk_of(bufs, k, step * LANES), (((1,), (1,)), ((), ())), preferred_element_type=jnp.float32
            )
            sums[i] = part if k == 0 else sums[i] + part
    return sums


def down_into(hidden, copies, wd_ref, out_ref):
    blocks, chips, cap, lanes = out_ref.shape
    step = chips // CHUNKS
    for k in range(CHUNKS):
        wait_all(copies[k * step : (k + 1) * step])
        part = dot32(hidden, wd_ref[:, k * step * lanes : (k + 1) * step * lanes]).astype(out_ref.dtype)
        for z in range(step):
            out_ref[:, k * step + z] = part[:, z * lanes : (z + 1) * lanes].reshape(blocks, cap, lanes)


def first_half_body(core_ref, x_ref, wg_ref, wu_ref, gate_ref, up_ref, g_ahead, u_ahead, g_buf, u_buf, sems, ahead_sems):
    core = core_ref[0]
    gates = core_copies(wg_ref, core, g_buf, sems.at[0])
    ups = core_copies(wu_ref, core, u_buf, sems.at[1])
    ahead = core_copies(wg_ref, 1 - core, g_ahead, ahead_sems.at[0])
    ahead += core_copies(wu_ref, 1 - core, u_ahead, ahead_sems.at[1])
    for pair in zip(gates, ups):
        start_all(pair)
    start_all(ahead)
    gate_ref[...], up_ref[...] = up_partial(x_ref, [(gates, [g_buf]), (ups, [u_buf])])
    wait_all(ahead)


def second_half_body(
    core_ref, x_ref, gate_ref, up_ref, g_ahead, u_ahead, wg_ref, wu_ref, wd_ref,
    hidden_ref, out_ref, down_own, g_buf, u_buf, d_buf, sems,
):
    core = core_ref[0]
    here = g_ahead.shape[1] // LANES
    gates = core_copies(wg_ref, 1 - core, g_buf, sems.at[0], here)
    ups = core_copies(wu_ref, 1 - core, u_buf, sems.at[1], here)
    downs = core_copies(wd_ref, 1 - core, d_buf, sems.at[2])
    owns = core_copies(wd_ref, core, down_own, sems.at[3])
    for pair in zip(gates, ups):
        start_all(pair)
    start_all(downs)
    start_all(owns)
    held = [None] * here
    gate, up = up_partial(x_ref, [(held + gates, [g_ahead, g_buf]), (held + ups, [u_ahead, u_buf])])
    gate = gate + gate_ref[...]
    up = up + up_ref[...]
    hidden = (gate / (1.0 + jnp.exp(-gate)) * up).astype(jnp.bfloat16)
    hidden_ref[...] = hidden
    down_into(hidden, downs, d_buf, out_ref)
    wait_all(owns)


def own_down_body(hidden_ref, down_own, out_ref):
    down_into(hidden_ref[...], [], down_own, out_ref)


def combine_body(parity_ref, table_ref, results_ref, own_ref, right_ref, left_ref):
    parity = parity_ref[0]
    table = table_ref[...]
    half = right_ref.shape[0]

    def rows_of(chip):
        return results_ref[:, chip].reshape(-1, LANES)

    for k in range(2 * half):
        mine, other = rows_of(PARITIES * k + parity), rows_of(PARITIES * k + 1 - parity)
        rows = dot32(table, jnp.concatenate([mine, other], axis=1)).astype(own_ref.dtype)
        own_ref[k] = rows[:, :LANES]
        (right_ref if k < half else left_ref)[k % half] = rows[:, LANES:]


def chip_pair_body(own_ref, low_ref, high_ref, out_ref):
    half = low_ref.shape[0]
    for part, ref in enumerate((low_ref, high_ref)):
        rows = pl.ds(part * half, half)
        out_ref[rows] = (own_ref[rows].astype(jnp.float32) + ref[...].astype(jnp.float32)).astype(out_ref.dtype)


def call(body, out_shape, in_specs, scratch=(), flops=0):
    outs = jax.tree.map(lambda _: VMEM, out_shape)
    return pl.pallas_call(
        body,
        out_shape=out_shape,
        in_specs=list(in_specs),
        out_specs=outs,
        scratch_shapes=list(scratch),
        cost_estimate=pl.CostEstimate(flops=flops, transcendentals=0, bytes_accessed=flops // 400),
        compiler_params=pltpu.CompilerParams(vmem_limit_bytes=24 * 1024 * 1024),
    )


def shards(tokens, route_ids, gate_weights, w_gate, w_up, w_down):
    experts = lax.axis_size("expert")
    chips = lax.axis_size(Z)
    token_count, lanes = tokens.shape
    slots = experts * CAP
    _, width_in, width = w_gate.shape
    bf16, f32 = jnp.bfloat16, jnp.float32
    shape = jax.ShapeDtypeStruct

    expert_iota = lax.broadcasted_iota(jnp.int32, (1, 1, experts), 2)
    hit_mask = route_ids[:, :, None] == expert_iota
    routed = jnp.any(hit_mask, axis=1).astype(jnp.int32)
    weighting = jnp.sum(jnp.where(hit_mask, gate_weights[:, :, None], 0.0), axis=1)
    slot_index = jnp.cumsum(routed, axis=0) - 1
    expert_base = lax.broadcasted_iota(jnp.int32, (1, experts), 1) * CAP
    target_slot = jnp.where(routed == 1, expert_base + slot_index, -1)
    slot_iota = lax.broadcasted_iota(jnp.int32, (1, 1, slots), 2)
    pick_table = target_slot[:, :, None] == slot_iota
    select_table = jnp.any(pick_table, axis=1).astype(bf16).T
    combine_table = jnp.sum(jnp.where(pick_table, weighting[:, :, None], 0.0), axis=1).astype(bf16)

    core = lax.axis_index("core").astype(jnp.int32).reshape(1)
    parity = lax.axis_index("z_1").astype(jnp.int32).reshape(1)
    select_table, combine_table, core, parity = lax.optimization_barrier((select_table, combine_table, core, parity))

    swap = functools.partial(lax.ppermute, axis_name="core", perm=[(0, 1), (1, 0)])
    exchange = functools.partial(lax.all_to_all, split_axis=0, concat_axis=0, tiled=True)

    gathered = lax.all_gather(tokens, Z, axis=0, tiled=False)
    sent = call(
        dispatch_body, shape((experts, chips, CAP, lanes), bf16), (VMEM, VMEM), flops=2 * slots * token_count * chips * lanes
    )(select_table, gathered)
    own = exchange(sent, "expert")
    other = swap(own)

    gate_rows, up_rows, down_rows = (
        pltpu.with_memory_space_constraint(w, pltpu.HBM)
        for w in (jnp.swapaxes(w_gate[0], 0, 1), jnp.swapaxes(w_up[0], 0, 1), w_down[0])
    )
    up_flops = 2 * slots * width * width_in
    acc = shape((slots, width), f32)
    ahead = shape((width, AHEAD * (chips // CHUNKS) * lanes), bf16)
    half_width = chips * lanes
    gate_half, up_half, gate_ahead, up_ahead = call(
        first_half_body,
        (acc, acc, ahead, ahead),
        (SMEM, VMEM, HBM, HBM),
        [pltpu.VMEM((width, half_width), bf16)] * 2 + [pltpu.SemaphoreType.DMA((2, chips)), pltpu.SemaphoreType.DMA((2, chips))],
        flops=up_flops,
    )(core, own, gate_rows, up_rows)
    rest = pltpu.VMEM((width, half_width - ahead.shape[1]), bf16)
    hidden, theirs, down_own = call(
        second_half_body,
        (
            shape((slots, width), bf16),
            shape((experts, chips, CAP, lanes), bf16),
            shape((width, half_width), bf16),
        ),
        (SMEM, VMEM, VMEM, VMEM, VMEM, VMEM, HBM, HBM, HBM),
        [rest, rest, pltpu.VMEM((width, half_width), bf16), pltpu.SemaphoreType.DMA((4, chips))],
        flops=up_flops * 3 // 2,
    )(core, other, gate_half, up_half, gate_ahead, up_ahead, gate_rows, up_rows, down_rows)
    arrived = swap(theirs)
    mine = call(own_down_body, shape((experts, chips, CAP, lanes), f32), (VMEM, VMEM), flops=up_flops // 2)(
        hidden, down_own
    )
    chip_sum = (mine + arrived.astype(f32)).astype(bf16)
    results = exchange(chip_sum, "expert")

    of_parity = chips // PARITIES

    def block(count):
        return shape((count, token_count, lanes), bf16)

    blended, right, left = call(
        combine_body,
        (block(of_parity), block(of_parity // 2), block(of_parity // 2)),
        (SMEM, VMEM, VMEM),
        flops=2 * slots * token_count * chips * lanes,
    )(parity, combine_table, results)
    low = lax.ppermute(right, Z, [(z, (z + 1) % chips) for z in range(chips)])
    high = lax.ppermute(left, Z, [(z, (z - 1) % chips) for z in range(chips)])
    paired = call(chip_pair_body, block(of_parity), (VMEM, VMEM, VMEM))(blended, low, high)
    pieces = exchange(paired, "z_0")
    return pieces.astype(f32).sum(axis=0).astype(bf16)


def solution(mesh):
    groups, experts, etp = (mesh.shape[name] for name in ("groups", "expert", "etp"))
    finer = Mesh(
        mesh.devices.reshape(groups, experts, etp // (CORES * PARITIES), PARITIES, CORES),
        ("groups", "expert", *ETP),
    )
    placed = (
        P(("groups", "expert"), ETP),
        P(("groups", "expert"), None),
        P(("groups", "expert"), None),
        P("expert", None, ETP),
        P("expert", None, ETP),
        P("expert", ETP, None),
    )
    return jax.shard_map(
        shards, mesh=finer, in_specs=placed, out_specs=P(("groups", "expert"), ETP), check_vma=False
    )
```

```python
import functools

import jax
import jax.numpy as jnp
from jax import lax
from jax.experimental import pallas as pl
from jax.experimental.pallas import tpu as pltpu
from jax.sharding import Mesh
from jax.sharding import PartitionSpec as P

CAP = 96
CORES = 2
Z = ("z_0", "z_1")
ETP = (*Z, "core")
LANES = 128
CHUNKS = 4
UNITS = 128
PARITIES = 2

HBM = pl.BlockSpec(memory_space=pltpu.HBM)
VMEM = pl.BlockSpec(memory_space=pltpu.VMEM)
SMEM = pl.BlockSpec(memory_space=pltpu.SMEM)


def dot32(a, b):
    return jnp.dot(a, b, preferred_element_type=jnp.float32)


def side_by_side(tiles):
    return jnp.concatenate([tile.reshape(-1, LANES) for tile in tiles], axis=1)


def slot_table(routes_ref, cap, experts, weight_of):
    tokens = routes_ref.shape[1]
    rows = -(-experts // 8) * 8
    expert = lax.broadcasted_iota(jnp.int32, (rows, tokens), 0)
    hit = (routes_ref[0:1, :] == expert) | (routes_ref[1:2, :] == expert)
    square = (tokens, tokens)
    earlier = lax.broadcasted_iota(jnp.int32, square, 0) < lax.broadcasted_iota(jnp.int32, square, 1)
    ones = [jnp.where(mask, 1.0, 0.0).astype(jnp.bfloat16) for mask in (hit, earlier)]
    slot = jnp.where(hit, dot32(*ones), -1.0).astype(jnp.int32)
    number = lax.broadcasted_iota(jnp.int32, (cap, tokens), 0)
    parts = [jnp.where(slot[e : e + 1, :] == number, weight_of(e), 0.0) for e in range(experts)]
    return jnp.concatenate(parts, axis=0).astype(jnp.bfloat16)


def dispatch_body(routes_ref, tokens_ref, out_ref):
    experts, chips, cap, lanes = out_ref.shape
    table = slot_table(routes_ref, cap, experts, lambda e: 1.0)
    for z in range(0, chips, 2):
        rows = dot32(table, side_by_side([tokens_ref[z], tokens_ref[z + 1]])).astype(out_ref.dtype)
        for k in range(2):
            out_ref[:, z + k] = rows[:, k * lanes : (k + 1) * lanes].reshape(experts, cap, lanes)


def row_copies(w_ref, buf, sems):
    width = w_ref.shape[0]
    spans = [pl.ds(k, min(UNITS, width - k)) for k in range(0, width, UNITS)]
    return [pltpu.make_async_copy(w_ref.at[span], buf.at[span], sems.at[i]) for i, span in enumerate(spans)]


def start_all(copies):
    for copy in copies:
        copy.start()


def wait_all(copies):
    for copy in copies:
        copy.wait()


def core_columns(ref, rows, core, start, count):
    return side_by_side(
        [ref[rows, pl.ds(pl.multiple_of((z * CORES + core) * LANES, LANES), LANES)] for z in range(start, start + count)]
    )


def up_partial(core, x_ref, gate_w, up_w, ready, emit):
    chips = x_ref.shape[1]
    width = gate_w.shape[0]
    x = side_by_side([x_ref[:, z] for z in range(chips)])
    for i, k in enumerate(range(0, width, UNITS)):
        rows = slice(k, min(k + UNITS, width))
        size = rows.stop - rows.start
        ready(i)
        both = jnp.concatenate([core_columns(w, rows, core, 0, chips) for w in (gate_w, up_w)], axis=0)
        part = lax.dot_general(x, both, (((1,), (1,)), ((), ())), preferred_element_type=jnp.float32)
        emit(rows, part[:, :size], part[:, size:])


def down_into(hidden, core, wd_ref, out_ref):
    blocks, chips, cap, lanes = out_ref.shape
    step = chips // CHUNKS
    for k in range(0, chips, step):
        part = dot32(hidden, core_columns(wd_ref, slice(None), core, k, step)).astype(out_ref.dtype)
        for z in range(step):
            out_ref[:, k + z] = part[:, z * lanes : (z + 1) * lanes].reshape(blocks, cap, lanes)


def first_half_body(
    core_ref, x_ref, routes_ref, weights_ref, wg_ref, wu_ref, gate_ref, up_ref, g_here, u_here, table_ref, sems
):
    gates = row_copies(wg_ref, g_here, sems.at[0])
    ups = row_copies(wu_ref, u_here, sems.at[1])
    for pair in zip(gates, ups):
        start_all(pair)

    def weight_of(e):
        return sum(jnp.where(routes_ref[k : k + 1, :] == e, weights_ref[k : k + 1, :], 0.0) for k in range(2))

    table_ref[...] = slot_table(routes_ref, x_ref.shape[2], x_ref.shape[0], weight_of).T

    def ready(i):
        wait_all((gates[i], ups[i]))

    def emit(rows, gate, up):
        gate_ref[:, rows], up_ref[:, rows] = gate, up

    up_partial(core_ref[0], x_ref, g_here, u_here, ready, emit)


def second_half_body(
    core_ref, x_ref, gate_ref, up_ref, g_here, u_here, wd_ref, hidden_ref, out_ref, d_here, sems
):
    other = 1 - core_ref[0]
    downs = row_copies(wd_ref, d_here, sems)
    start_all(downs)

    def emit(rows, gate, up):
        gate = gate + gate_ref[:, rows]
        up = up + up_ref[:, rows]
        hidden_ref[:, rows] = (gate / (1.0 + jnp.exp(-gate)) * up).astype(hidden_ref.dtype)

    up_partial(other, x_ref, g_here, u_here, lambda i: None, emit)
    wait_all(downs)
    down_into(hidden_ref[...], other, d_here, out_ref)


def own_down_body(core_ref, hidden_ref, d_here, out_ref):
    down_into(hidden_ref[...], core_ref[0], d_here, out_ref)


def combine_body(parity_ref, table_ref, results_ref, own_ref, right_ref, left_ref):
    parity = parity_ref[0]
    table = table_ref[...]
    half = right_ref.shape[0]

    def rows_of(chip):
        return results_ref[:, chip].reshape(-1, LANES)

    for k in range(2 * half):
        mine, other = rows_of(PARITIES * k + parity), rows_of(PARITIES * k + 1 - parity)
        rows = dot32(table, jnp.concatenate([mine, other], axis=1)).astype(own_ref.dtype)
        own_ref[k] = rows[:, :LANES]
        (right_ref if k < half else left_ref)[k % half] = rows[:, LANES:]


def chip_pair_body(own_ref, low_ref, high_ref, out_ref):
    half = low_ref.shape[0]
    for part, ref in enumerate((low_ref, high_ref)):
        rows = pl.ds(part * half, half)
        out_ref[rows] = (own_ref[rows].astype(jnp.float32) + ref[...].astype(jnp.float32)).astype(out_ref.dtype)


def call(body, out_shape, in_specs, scratch=(), flops=0):
    outs = jax.tree.map(lambda _: VMEM, out_shape)
    return pl.pallas_call(
        body,
        out_shape=out_shape,
        in_specs=list(in_specs),
        out_specs=outs,
        scratch_shapes=list(scratch),
        cost_estimate=pl.CostEstimate(flops=flops, transcendentals=0, bytes_accessed=flops // 400),
        compiler_params=pltpu.CompilerParams(vmem_limit_bytes=24 * 1024 * 1024),
    )


def shards(tokens, route_ids, gate_weights, w_gate, w_up, w_down):
    experts = lax.axis_size("expert")
    chips = lax.axis_size(Z)
    token_count, lanes = tokens.shape
    slots = experts * CAP
    _, width_in, width = w_gate.shape
    bf16, f32 = jnp.bfloat16, jnp.float32
    shape = jax.ShapeDtypeStruct

    routes, weights = route_ids.T, gate_weights.T
    core = lax.axis_index("core").astype(jnp.int32).reshape(1)
    parity = lax.axis_index("z_1").astype(jnp.int32).reshape(1)
    tokens, core, parity = lax.optimization_barrier((tokens, core, parity))

    swap = functools.partial(lax.ppermute, axis_name="core", perm=[(0, 1), (1, 0)])
    exchange = functools.partial(lax.all_to_all, split_axis=0, concat_axis=0, tiled=True)

    gathered = lax.all_gather(tokens, Z, axis=0, tiled=False)
    sent = call(
        dispatch_body, shape((experts, chips, CAP, lanes), bf16), (VMEM, VMEM), flops=2 * slots * token_count * chips * lanes
    )(routes, gathered)
    own = exchange(sent, "expert")
    other = swap(own)

    gate_rows, up_rows, down_rows = (
        pltpu.with_memory_space_constraint(w, pltpu.HBM)
        for w in (jnp.swapaxes(w_gate[0], 0, 1), jnp.swapaxes(w_up[0], 0, 1), w_down[0])
    )
    up_flops = 2 * slots * width * width_in
    acc = shape((slots, width), f32)
    held = shape((width, width_in), bf16)
    copies = len(range(0, width, UNITS))
    gate_half, up_half, gate_here, up_here, combine_table = call(
        first_half_body,
        (acc, acc, held, held, shape((token_count, slots), bf16)),
        (SMEM, VMEM, VMEM, VMEM, HBM, HBM),
        [pltpu.SemaphoreType.DMA((2, copies))],
        flops=up_flops,
    )(core, own, routes, weights, gate_rows, up_rows)
    hidden, theirs, down_here = call(
        second_half_body,
        (shape((slots, width), bf16), shape((experts, chips, CAP, lanes), bf16), held),
        (SMEM, VMEM, VMEM, VMEM, VMEM, VMEM, HBM),
        [pltpu.SemaphoreType.DMA((copies,))],
        flops=up_flops * 3 // 2,
    )(core, other, gate_half, up_half, gate_here, up_here, down_rows)
    arrived = swap(theirs)
    mine = call(own_down_body, shape((experts, chips, CAP, lanes), f32), (SMEM, VMEM, VMEM), flops=up_flops // 2)(
        core, hidden, down_here
    )
    chip_sum = (mine + arrived.astype(f32)).astype(bf16)
    results = exchange(chip_sum, "expert")

    of_parity = chips // PARITIES

    def block(count):
        return shape((count, token_count, lanes), bf16)

    blended, right, left = call(
        combine_body,
        (block(of_parity), block(of_parity // 2), block(of_parity // 2)),
        (SMEM, VMEM, VMEM),
        flops=2 * slots * token_count * chips * lanes,
    )(parity, combine_table, results)
    low = lax.ppermute(right, Z, [(z, (z + 1) % chips) for z in range(chips)])
    high = lax.ppermute(left, Z, [(z, (z - 1) % chips) for z in range(chips)])
    paired = call(chip_pair_body, block(of_parity), (VMEM, VMEM, VMEM))(blended, low, high)
    pieces = exchange(paired, "z_0")
    return pieces.astype(f32).sum(axis=0).astype(bf16)


def solution(mesh):
    groups, experts, etp = (mesh.shape[name] for name in ("groups", "expert", "etp"))
    finer = Mesh(
        mesh.devices.reshape(groups, experts, etp // (CORES * PARITIES), PARITIES, CORES),
        ("groups", "expert", *ETP),
    )
    placed = (
        P(("groups", "expert"), ETP),
        P(("groups", "expert"), None),
        P(("groups", "expert"), None),
        P("expert", None, ETP),
        P("expert", None, ETP),
        P("expert", ETP, None),
    )
    return jax.shard_map(
        shards, mesh=finer, in_specs=placed, out_specs=P(("groups", "expert"), ETP), check_vma=False
    )
```

```python
import functools

import jax
import jax.numpy as jnp
from jax import lax
from jax.experimental import pallas as pl
from jax.experimental.pallas import tpu as pltpu
from jax.sharding import Mesh
from jax.sharding import PartitionSpec as P

CAP = 96
CORES = 2
Z = ("z_0", "z_1")
ETP = (*Z, "core")
LANES = 128
CHUNKS = 4
PARITIES = 2

HBM = pl.BlockSpec(memory_space=pltpu.HBM)
VMEM = pl.BlockSpec(memory_space=pltpu.VMEM)
SMEM = pl.BlockSpec(memory_space=pltpu.SMEM)


def dot32(a, b):
    return jnp.dot(a, b, preferred_element_type=jnp.float32)


def side_by_side(tiles):
    return jnp.concatenate([tile.reshape(-1, LANES) for tile in tiles], axis=1)


def slot_table(routes_ref, cap, experts, weight_of):
    tokens = routes_ref.shape[1]
    rows = -(-experts // 8) * 8
    expert = lax.broadcasted_iota(jnp.int32, (rows, tokens), 0)
    hit = (routes_ref[0:1, :] == expert) | (routes_ref[1:2, :] == expert)
    square = (tokens, tokens)
    earlier = lax.broadcasted_iota(jnp.int32, square, 0) < lax.broadcasted_iota(jnp.int32, square, 1)
    ones = [jnp.where(mask, 1.0, 0.0).astype(jnp.bfloat16) for mask in (hit, earlier)]
    slot = jnp.where(hit, dot32(*ones), -1.0).astype(jnp.int32)
    number = lax.broadcasted_iota(jnp.int32, (cap, tokens), 0)
    parts = [jnp.where(slot[e : e + 1, :] == number, weight_of(e), 0.0) for e in range(experts)]
    return jnp.concatenate(parts, axis=0).astype(jnp.bfloat16)


def dispatch_body(routes_ref, tokens_ref, out_ref):
    experts, chips, cap, lanes = out_ref.shape
    table = slot_table(routes_ref, cap, experts, lambda e: 1.0)
    for z in range(0, chips, 2):
        rows = dot32(table, side_by_side([tokens_ref[z], tokens_ref[z + 1]])).astype(out_ref.dtype)
        for k in range(2):
            out_ref[:, z + k] = rows[:, k * lanes : (k + 1) * lanes].reshape(experts, cap, lanes)


def column_copies(w_ref, buf, sems):
    step = w_ref.shape[1] // CHUNKS
    spans = [pl.ds(k * step, step) for k in range(CHUNKS)]
    return [pltpu.make_async_copy(w_ref.at[:, span], buf.at[:, span], sems.at[i]) for i, span in enumerate(spans)]


def start_all(copies):
    for copy in copies:
        copy.start()


def wait_all(copies):
    for copy in copies:
        copy.wait()


def core_columns(ref, core, start, count):
    return side_by_side(
        [ref[:, pl.ds(pl.multiple_of((z * CORES + core) * LANES, LANES), LANES)] for z in range(start, start + count)]
    )


def up_partial(core, x_ref, w_refs, ready):
    step = x_ref.shape[1] // CHUNKS
    sums = [None] * len(w_refs)
    for k in range(CHUNKS):
        ready(k)
        x = side_by_side([x_ref[:, z] for z in range(k * step, (k + 1) * step)])
        for i, w in enumerate(w_refs):
            part = lax.dot_general(
                x, core_columns(w, core, k * step, step), (((1,), (1,)), ((), ())), preferred_element_type=jnp.float32
            )
            sums[i] = part if k == 0 else sums[i] + part
    return sums


def down_into(hidden, core, wd_ref, out_ref, ready=None):
    blocks, chips, cap, lanes = out_ref.shape
    step = chips // CHUNKS
    for k in range(CHUNKS):
        if ready is not None:
            ready(k)
        part = dot32(hidden, core_columns(wd_ref, core, k * step, step)).astype(out_ref.dtype)
        for z in range(step):
            out_ref[:, k * step + z] = part[:, z * lanes : (z + 1) * lanes].reshape(blocks, cap, lanes)


def first_half_body(
    core_ref, x_ref, routes_ref, weights_ref, wg_ref, wu_ref, gate_ref, up_ref, g_here, u_here, table_ref, sems
):
    gates = column_copies(wg_ref, g_here, sems.at[0])
    ups = column_copies(wu_ref, u_here, sems.at[1])
    for pair in zip(gates, ups):
        start_all(pair)

    def weight_of(e):
        return sum(jnp.where(routes_ref[k : k + 1, :] == e, weights_ref[k : k + 1, :], 0.0) for k in range(2))

    table_ref[...] = slot_table(routes_ref, x_ref.shape[2], x_ref.shape[0], weight_of).T

    gate_ref[...], up_ref[...] = up_partial(
        core_ref[0], x_ref, (g_here, u_here), lambda k: wait_all((gates[k], ups[k]))
    )


def second_half_body(
    core_ref, x_ref, gate_ref, up_ref, g_here, u_here, wd_ref, hidden_ref, out_ref, d_here, sems
):
    other = 1 - core_ref[0]
    downs = column_copies(wd_ref, d_here, sems)
    start_all(downs)
    gate, up = up_partial(other, x_ref, (g_here, u_here), lambda k: None)
    gate = gate + gate_ref[...]
    up = up + up_ref[...]
    hidden = (gate / (1.0 + jnp.exp(-gate)) * up).astype(hidden_ref.dtype)
    hidden_ref[...] = hidden
    down_into(hidden, other, d_here, out_ref, lambda k: downs[k].wait())


def own_down_body(core_ref, hidden_ref, d_here, out_ref):
    down_into(hidden_ref[...], core_ref[0], d_here, out_ref)


def combine_body(parity_ref, table_ref, results_ref, own_ref, right_ref, left_ref):
    parity = parity_ref[0]
    table = table_ref[...]
    half = right_ref.shape[0]

    def rows_of(chip):
        return results_ref[:, chip].reshape(-1, LANES)

    for k in range(2 * half):
        mine, other = rows_of(PARITIES * k + parity), rows_of(PARITIES * k + 1 - parity)
        rows = dot32(table, jnp.concatenate([mine, other], axis=1)).astype(own_ref.dtype)
        own_ref[k] = rows[:, :LANES]
        (right_ref if k < half else left_ref)[k % half] = rows[:, LANES:]


def chip_pair_body(own_ref, low_ref, high_ref, out_ref):
    half = low_ref.shape[0]
    for part, ref in enumerate((low_ref, high_ref)):
        rows = pl.ds(part * half, half)
        out_ref[rows] = (own_ref[rows].astype(jnp.float32) + ref[...].astype(jnp.float32)).astype(out_ref.dtype)


def call(body, out_shape, in_specs, scratch=(), flops=0):
    outs = jax.tree.map(lambda _: VMEM, out_shape)
    return pl.pallas_call(
        body,
        out_shape=out_shape,
        in_specs=list(in_specs),
        out_specs=outs,
        scratch_shapes=list(scratch),
        cost_estimate=pl.CostEstimate(flops=flops, transcendentals=0, bytes_accessed=flops // 400),
        compiler_params=pltpu.CompilerParams(vmem_limit_bytes=24 * 1024 * 1024),
    )


def shards(tokens, route_ids, gate_weights, w_gate, w_up, w_down):
    experts = lax.axis_size("expert")
    chips = lax.axis_size(Z)
    token_count, lanes = tokens.shape
    slots = experts * CAP
    _, width_in, width = w_gate.shape
    bf16, f32 = jnp.bfloat16, jnp.float32
    shape = jax.ShapeDtypeStruct

    routes, weights = route_ids.T, gate_weights.T
    core = lax.axis_index("core").astype(jnp.int32).reshape(1)
    parity = lax.axis_index("z_1").astype(jnp.int32).reshape(1)
    tokens, core, parity = lax.optimization_barrier((tokens, core, parity))

    swap = functools.partial(lax.ppermute, axis_name="core", perm=[(0, 1), (1, 0)])
    exchange = functools.partial(lax.all_to_all, split_axis=0, concat_axis=0, tiled=True)

    gathered = lax.all_gather(tokens, Z, axis=0, tiled=False)
    sent = call(
        dispatch_body, shape((experts, chips, CAP, lanes), bf16), (VMEM, VMEM), flops=2 * slots * token_count * chips * lanes
    )(routes, gathered)
    own = exchange(sent, "expert")
    other = swap(own)

    gate_rows, up_rows, down_rows = (
        pltpu.with_memory_space_constraint(w, pltpu.HBM)
        for w in (jnp.swapaxes(w_gate[0], 0, 1), jnp.swapaxes(w_up[0], 0, 1), w_down[0])
    )
    up_flops = 2 * slots * width * width_in
    acc = shape((slots, width), f32)
    held = shape((width, width_in), bf16)
    gate_half, up_half, gate_here, up_here, combine_table = call(
        first_half_body,
        (acc, acc, held, held, shape((token_count, slots), bf16)),
        (SMEM, VMEM, VMEM, VMEM, HBM, HBM),
        [pltpu.SemaphoreType.DMA((2, CHUNKS))],
        flops=up_flops,
    )(core, own, routes, weights, gate_rows, up_rows)
    hidden, theirs, down_here = call(
        second_half_body,
        (shape((slots, width), bf16), shape((experts, chips, CAP, lanes), bf16), held),
        (SMEM, VMEM, VMEM, VMEM, VMEM, VMEM, HBM),
        [pltpu.SemaphoreType.DMA((CHUNKS,))],
        flops=up_flops * 3 // 2,
    )(core, other, gate_half, up_half, gate_here, up_here, down_rows)
    arrived = swap(theirs)
    mine = call(own_down_body, shape((experts, chips, CAP, lanes), f32), (SMEM, VMEM, VMEM), flops=up_flops // 2)(
        core, hidden, down_here
    )
    chip_sum = (mine + arrived.astype(f32)).astype(bf16)
    results = exchange(chip_sum, "expert")

    of_parity = chips // PARITIES

    def block(count):
        return shape((count, token_count, lanes), bf16)

    blended, right, left = call(
        combine_body,
        (block(of_parity), block(of_parity // 2), block(of_parity // 2)),
        (SMEM, VMEM, VMEM),
        flops=2 * slots * token_count * chips * lanes,
    )(parity, combine_table, results)
    low = lax.ppermute(right, Z, [(z, (z + 1) % chips) for z in range(chips)])
    high = lax.ppermute(left, Z, [(z, (z - 1) % chips) for z in range(chips)])
    paired = call(chip_pair_body, block(of_parity), (VMEM, VMEM, VMEM))(blended, low, high)
    pieces = exchange(paired, "z_0")
    return pieces.astype(f32).sum(axis=0).astype(bf16)


def solution(mesh):
    groups, experts, etp = (mesh.shape[name] for name in ("groups", "expert", "etp"))
    finer = Mesh(
        mesh.devices.reshape(groups, experts, etp // (CORES * PARITIES), PARITIES, CORES),
        ("groups", "expert", *ETP),
    )
    placed = (
        P(("groups", "expert"), ETP),
        P(("groups", "expert"), None),
        P(("groups", "expert"), None),
        P("expert", None, ETP),
        P("expert", None, ETP),
        P("expert", ETP, None),
    )
    return jax.shard_map(
        shards, mesh=finer, in_specs=placed, out_specs=P(("groups", "expert"), ETP), check_vma=False
    )
```

```python
import functools

import jax
import jax.numpy as jnp
from jax import lax
from jax.experimental import pallas as pl
from jax.experimental.pallas import tpu as pltpu
from jax.sharding import Mesh
from jax.sharding import PartitionSpec as P

CAP = 96
CORES = 2
Z = ("z_0", "z_1")
ETP = (*Z, "core")
LANES = 128
CHUNKS = 4
TOP = 12
LEVELS = 14
MARK_ROWS = 8
PARITIES = 2

HBM = pl.BlockSpec(memory_space=pltpu.HBM)
VMEM = pl.BlockSpec(memory_space=pltpu.VMEM)
SMEM = pl.BlockSpec(memory_space=pltpu.SMEM)


def dot32(a, b):
    return jnp.dot(a, b, preferred_element_type=jnp.float32)


def side_by_side(tiles):
    return jnp.concatenate([tile.reshape(-1, LANES) for tile in tiles], axis=1)


def slot_table(routes_ref, cap, experts, weight_of):
    tokens = routes_ref.shape[1]
    rows = -(-experts // 8) * 8
    expert = lax.broadcasted_iota(jnp.int32, (rows, tokens), 0)
    hit = (routes_ref[0:1, :] == expert) | (routes_ref[1:2, :] == expert)
    square = (tokens, tokens)
    earlier = lax.broadcasted_iota(jnp.int32, square, 0) < lax.broadcasted_iota(jnp.int32, square, 1)
    ones = [jnp.where(mask, 1.0, 0.0).astype(jnp.bfloat16) for mask in (hit, earlier)]
    slot = jnp.where(hit, dot32(*ones), -1.0).astype(jnp.int32)
    number = lax.broadcasted_iota(jnp.int32, (cap, tokens), 0)
    parts = [jnp.where(slot[e : e + 1, :] == number, weight_of(e), 0.0) for e in range(experts)]
    return jnp.concatenate(parts, axis=0).astype(jnp.bfloat16)


def dispatch_body(routes_ref, tokens_ref, out_ref):
    experts, rows, lanes = out_ref.shape
    tokens = tokens_ref[...]
    largest = jnp.max(jnp.abs(tokens.astype(jnp.float32)))
    scale, mark = jnp.float32(2.0**TOP), jnp.float32(1.0)
    for level in range(1, LEVELS):
        lower = largest < 2.0 ** (15 - TOP - 8 * level)
        scale = jnp.where(lower, 2.0 ** (TOP + 8 * level), scale)
        mark = jnp.where(lower, 2.0**-level, mark)
    picked = dot32(slot_table(routes_ref, CAP, experts, lambda e: 1.0), tokens) * scale
    out_ref[:, :CAP] = picked.astype(out_ref.dtype).reshape(experts, CAP, lanes)
    out_ref[:, CAP:] = jnp.full((experts, rows - CAP, lanes), mark, jnp.float32).astype(out_ref.dtype)


def unscaled(tile_ref, z):
    mark = tile_ref[z, :, CAP : CAP + 1].astype(jnp.float32)
    for _ in range(3):
        mark = mark * mark
    return tile_ref[z, :, :CAP] * (mark * 2.0**-TOP).astype(tile_ref.dtype)


def column_copies(w_ref, buf, sems):
    step = w_ref.shape[1] // CHUNKS
    spans = [pl.ds(k * step, step) for k in range(CHUNKS)]
    return [pltpu.make_async_copy(w_ref.at[:, span], buf.at[:, span], sems.at[i]) for i, span in enumerate(spans)]


def core_columns(ref, core, start, count):
    return side_by_side(
        [ref[:, pl.ds(pl.multiple_of((z * CORES + core) * LANES, LANES), LANES)] for z in range(start, start + count)]
    )


def up_partial(core, x_ref, w_ref, copies=None):
    step = x_ref.shape[0] // CHUNKS
    total = None
    for k in range(CHUNKS):
        x = side_by_side([unscaled(x_ref, z) for z in range(k * step, (k + 1) * step)])
        if copies is not None:
            copies[k].wait()
        part = lax.dot_general(
            x, core_columns(w_ref, core, k * step, step), (((1,), (1,)), ((), ())), preferred_element_type=jnp.float32
        )
        total = part if k == 0 else total + part
    return total


def down_into(hidden, core, wd_ref, out_ref):
    blocks, chips, cap, lanes = out_ref.shape
    step = chips // CHUNKS
    for k in range(CHUNKS):
        part = dot32(hidden, core_columns(wd_ref, core, k * step, step)).astype(out_ref.dtype)
        for z in range(step):
            out_ref[:, k * step + z] = part[:, z * lanes : (z + 1) * lanes].reshape(blocks, cap, lanes)


def first_half_body(
    core_ref, x_ref, routes_ref, weights_ref, wg_ref, wu_ref, gate_ref, up_ref, u_here, table_ref, sems
):
    copies = column_copies(wu_ref, u_here, sems)
    for copy in copies:
        copy.start()

    def weight_of(e):
        return sum(jnp.where(routes_ref[k : k + 1, :] == e, weights_ref[k : k + 1, :], 0.0) for k in range(2))

    table_ref[...] = slot_table(routes_ref, CAP, x_ref.shape[1], weight_of).T
    gate_ref[...] = up_partial(core_ref[0], x_ref, wg_ref)
    up_ref[...] = up_partial(core_ref[0], x_ref, u_here, copies)


def second_half_body(core_ref, x_ref, gate_ref, up_ref, wg_ref, wu_ref, wd_ref, hidden_ref, out_ref):
    other = 1 - core_ref[0]
    gate = up_partial(other, x_ref, wg_ref) + gate_ref[...]
    up = up_partial(other, x_ref, wu_ref) + up_ref[...]
    hidden = (gate / (1.0 + jnp.exp(-gate)) * up).astype(hidden_ref.dtype)
    hidden_ref[...] = hidden
    down_into(hidden, other, wd_ref, out_ref)


def own_down_body(core_ref, hidden_ref, d_here, out_ref):
    down_into(hidden_ref[...], core_ref[0], d_here, out_ref)


def combine_body(parity_ref, table_ref, results_ref, own_ref, right_ref, left_ref):
    parity = parity_ref[0]
    table = table_ref[...]
    half = right_ref.shape[0]

    def rows_of(chip):
        return results_ref[:, chip].reshape(-1, LANES)

    for k in range(2 * half):
        mine, other = rows_of(PARITIES * k + parity), rows_of(PARITIES * k + 1 - parity)
        rows = dot32(table, jnp.concatenate([mine, other], axis=1)).astype(own_ref.dtype)
        own_ref[k] = rows[:, :LANES]
        (right_ref if k < half else left_ref)[k % half] = rows[:, LANES:]


def chip_pair_body(own_ref, low_ref, high_ref, out_ref):
    half = low_ref.shape[0]
    for part, ref in enumerate((low_ref, high_ref)):
        rows = pl.ds(part * half, half)
        out_ref[rows] = (own_ref[rows].astype(jnp.float32) + ref[...].astype(jnp.float32)).astype(out_ref.dtype)


def call(body, out_shape, in_specs, scratch=(), flops=0):
    outs = jax.tree.map(lambda _: VMEM, out_shape)
    return pl.pallas_call(
        body,
        out_shape=out_shape,
        in_specs=list(in_specs),
        out_specs=outs,
        scratch_shapes=list(scratch),
        cost_estimate=pl.CostEstimate(flops=flops, transcendentals=0, bytes_accessed=flops // 400),
        compiler_params=pltpu.CompilerParams(vmem_limit_bytes=16 * 1024 * 1024),
    )


def shards(tokens, route_ids, gate_weights, w_gate, w_up, w_down):
    experts = lax.axis_size("expert")
    chips = lax.axis_size(Z)
    token_count, lanes = tokens.shape
    slots = experts * CAP
    _, width_in, width = w_gate.shape
    bf16, f32 = jnp.bfloat16, jnp.float32
    shape = jax.ShapeDtypeStruct

    routes, weights = route_ids.T, gate_weights.T
    core = lax.axis_index("core").astype(jnp.int32).reshape(1)
    parity = lax.axis_index("z_1").astype(jnp.int32).reshape(1)
    tokens, core, parity = lax.optimization_barrier((tokens, core, parity))

    swap = functools.partial(lax.ppermute, axis_name="core", perm=[(0, 1), (1, 0)])
    exchange = functools.partial(lax.all_to_all, split_axis=0, concat_axis=0, tiled=True)

    picked = call(dispatch_body, shape((experts, CAP + MARK_ROWS, lanes), bf16), (VMEM, VMEM))(routes, tokens)
    slices = exchange(picked.astype(jnp.float16), "expert")
    own = lax.all_gather(slices, Z, axis=0, tiled=False).astype(bf16)
    other = swap(own)

    gate_rows, up_rows, down_rows = w_gate[0].T, w_up[0].T, w_down[0]
    up_rows = pltpu.with_memory_space_constraint(up_rows, pltpu.HBM)
    up_flops = 2 * slots * width * width_in
    acc = shape((slots, width), f32)
    gate_half, up_half, up_here, combine_table = call(
        first_half_body,
        (acc, acc, shape((width, width_in), bf16), shape((token_count, slots), bf16)),
        (SMEM, VMEM, VMEM, VMEM, VMEM, HBM),
        [pltpu.SemaphoreType.DMA((CHUNKS,))],
        flops=up_flops,
    )(core, own, routes, weights, gate_rows, up_rows)
    hidden, theirs = call(
        second_half_body,
        (shape((slots, width), bf16), shape((experts, chips, CAP, lanes), bf16)),
        (SMEM, VMEM, VMEM, VMEM, VMEM, VMEM, VMEM),
        flops=up_flops * 3 // 2,
    )(core, other, gate_half, up_half, gate_rows, up_here, down_rows)
    arrived = swap(theirs)
    mine = call(own_down_body, shape((experts, chips, CAP, lanes), f32), (SMEM, VMEM, VMEM), flops=up_flops // 2)(
        core, hidden, down_rows
    )
    chip_sum = (mine + arrived.astype(f32)).astype(bf16)
    results = exchange(chip_sum, "expert")

    of_parity = chips // PARITIES

    def block(count):
        return shape((count, token_count, lanes), bf16)

    blended, right, left = call(
        combine_body,
        (block(of_parity), block(of_parity // 2), block(of_parity // 2)),
        (SMEM, VMEM, VMEM),
        flops=2 * slots * token_count * chips * lanes,
    )(parity, combine_table, results)
    low = lax.ppermute(right, Z, [(z, (z + 1) % chips) for z in range(chips)])
    high = lax.ppermute(left, Z, [(z, (z - 1) % chips) for z in range(chips)])
    paired = call(chip_pair_body, block(of_parity), (VMEM, VMEM, VMEM))(blended, low, high)
    pieces = exchange(paired, "z_0")
    return pieces.astype(f32).sum(axis=0).astype(bf16)


def solution(mesh):
    groups, experts, etp = (mesh.shape[name] for name in ("groups", "expert", "etp"))
    finer = Mesh(
        mesh.devices.reshape(groups, experts, etp // (CORES * PARITIES), PARITIES, CORES),
        ("groups", "expert", *ETP),
    )
    placed = (
        P(("groups", "expert"), ETP),
        P(("groups", "expert"), None),
        P(("groups", "expert"), None),
        P("expert", None, ETP),
        P("expert", None, ETP),
        P("expert", ETP, None),
    )
    return jax.shard_map(
        shards, mesh=finer, in_specs=placed, out_specs=P(("groups", "expert"), ETP), check_vma=False
    )
```

```python
import functools

import jax
import jax.numpy as jnp
from jax import lax
from jax.experimental import pallas as pl
from jax.experimental.pallas import tpu as pltpu
from jax.sharding import Mesh
from jax.sharding import PartitionSpec as P

CAP = 96
CORES = 2
Z = ("z_0", "z_1")
ETP = (*Z, "core")
LANES = 128
CHUNKS = 4
TOP = 12
LEVELS = 14
MARK_ROWS = 8
PARITIES = 2

HBM = pl.BlockSpec(memory_space=pltpu.HBM)
VMEM = pl.BlockSpec(memory_space=pltpu.VMEM)
SMEM = pl.BlockSpec(memory_space=pltpu.SMEM)


def dot32(a, b):
    return jnp.dot(a, b, preferred_element_type=jnp.float32)


def side_by_side(tiles):
    return jnp.concatenate([tile.reshape(-1, LANES) for tile in tiles], axis=1)


def slot_table(routes_ref, cap, experts, weight_of):
    tokens = routes_ref.shape[1]
    rows = -(-experts // 8) * 8
    expert = lax.broadcasted_iota(jnp.int32, (rows, tokens), 0)
    hit = (routes_ref[0:1, :] == expert) | (routes_ref[1:2, :] == expert)
    square = (tokens, tokens)
    earlier = lax.broadcasted_iota(jnp.int32, square, 0) < lax.broadcasted_iota(jnp.int32, square, 1)
    ones = [jnp.where(mask, 1.0, 0.0).astype(jnp.bfloat16) for mask in (hit, earlier)]
    slot = jnp.where(hit, dot32(*ones), -1.0).astype(jnp.int32)
    number = lax.broadcasted_iota(jnp.int32, (cap, tokens), 0)
    parts = [jnp.where(slot[e : e + 1, :] == number, weight_of(e), 0.0) for e in range(experts)]
    return jnp.concatenate(parts, axis=0).astype(jnp.bfloat16)


def dispatch_body(routes_ref, tokens_ref, out_ref):
    experts, rows, lanes = out_ref.shape
    tokens = tokens_ref[...]
    largest = jnp.max(jnp.abs(tokens.astype(jnp.float32)))
    scale, mark = jnp.float32(2.0**TOP), jnp.float32(1.0)
    for level in range(1, LEVELS):
        lower = largest < 2.0 ** (15 - TOP - 8 * level)
        scale = jnp.where(lower, 2.0 ** (TOP + 8 * level), scale)
        mark = jnp.where(lower, 2.0**-level, mark)
    picked = dot32(slot_table(routes_ref, CAP, experts, lambda e: 1.0), tokens) * scale
    out_ref[:, :CAP] = picked.astype(out_ref.dtype).reshape(experts, CAP, lanes)
    out_ref[:, CAP:] = jnp.full((experts, rows - CAP, lanes), mark, jnp.float32).astype(out_ref.dtype)


def unscaled(tile_ref, z):
    mark = tile_ref[z, :, CAP : CAP + 1].astype(jnp.float32)
    for _ in range(3):
        mark = mark * mark
    return tile_ref[z, :, :CAP] * (mark * 2.0**-TOP).astype(tile_ref.dtype)


def column_copies(w_ref, buf, sems):
    step = w_ref.shape[1] // CHUNKS
    spans = [pl.ds(k * step, step) for k in range(CHUNKS)]
    return [pltpu.make_async_copy(w_ref.at[:, span], buf.at[:, span], sems.at[i]) for i, span in enumerate(spans)]


def core_columns(ref, core, chips):
    return side_by_side([ref[:, pl.ds(pl.multiple_of((z * CORES + core) * LANES, LANES), LANES)] for z in chips])


def up_partial(core, x_ref, w_ref, copies=None):
    step = x_ref.shape[0] // CHUNKS
    total = None
    for k in range(CHUNKS):
        x = side_by_side([unscaled(x_ref, z) for z in range(k * step, (k + 1) * step)])
        if copies is not None:
            copies[k].wait()
        part = lax.dot_general(
            x, core_columns(w_ref, core, range(k * step, (k + 1) * step)), (((1,), (1,)), ((), ())), preferred_element_type=jnp.float32
        )
        total = part if k == 0 else total + part
    return total


def down_into(hidden, core, parity, wd_ref, out_ref):
    blocks, count, cap, lanes = out_ref.shape
    step = 4
    for k in range(0, count, step):
        chips = [PARITIES * z + parity for z in range(k, k + step)]
        part = dot32(hidden, core_columns(wd_ref, core, chips)).astype(out_ref.dtype)
        for z in range(step):
            out_ref[:, k + z] = part[:, z * lanes : (z + 1) * lanes].reshape(blocks, cap, lanes)


def first_half_body(
    place_ref, x_ref, routes_ref, weights_ref, wg_ref, wu_ref, gate_ref, up_ref, u_here, table_ref, sems
):
    copies = column_copies(wu_ref, u_here, sems)
    for copy in copies:
        copy.start()

    def weight_of(e):
        return sum(jnp.where(routes_ref[k : k + 1, :] == e, weights_ref[k : k + 1, :], 0.0) for k in range(2))

    table_ref[...] = slot_table(routes_ref, CAP, x_ref.shape[1], weight_of).T
    gate_ref[...] = up_partial(place_ref[0], x_ref, wg_ref)
    up_ref[...] = up_partial(place_ref[0], x_ref, u_here, copies)


def second_half_body(place_ref, x_ref, gate_ref, up_ref, wg_ref, wu_ref, wd_ref, hidden_ref, out_ref):
    core, parity = place_ref[0], place_ref[1]
    gate = up_partial(1 - core, x_ref, wg_ref) + gate_ref[...]
    up = up_partial(1 - core, x_ref, wu_ref) + up_ref[...]
    hidden = (gate / (1.0 + jnp.exp(-gate)) * up).astype(hidden_ref.dtype)
    hidden_ref[...] = hidden
    down_into(hidden, 1 - core, 1 - parity, wd_ref, out_ref)


def down_body(place_ref, hidden_ref, wd_ref, out_ref, *, own_core, own_parity):
    core, parity = place_ref[0], place_ref[1]
    down_into(
        hidden_ref[...], core if own_core else 1 - core, parity if own_parity else 1 - parity, wd_ref, out_ref
    )


def outgoing_body(mine_ref, arrived_ref, right_ref, left_ref):
    half = right_ref.shape[1]
    for part, ref in enumerate((right_ref, left_ref)):
        chips = pl.ds(part * half, half)
        ref[...] = (mine_ref[:, chips] + arrived_ref[:, chips].astype(jnp.float32)).astype(ref.dtype)


def pair_body(mine_ref, arrived_ref, low_ref, high_ref, out_ref):
    half = low_ref.shape[1]
    for part, ref in enumerate((low_ref, high_ref)):
        chips = pl.ds(part * half, half)
        total = mine_ref[:, chips] + arrived_ref[:, chips].astype(jnp.float32) + ref[...].astype(jnp.float32)
        out_ref[:, chips] = total.astype(out_ref.dtype)


def combine_body(table_ref, results_ref, out_ref):
    chips, _, lanes = out_ref.shape
    table = table_ref[...]
    for z in range(0, chips, 2):
        rows = dot32(table, side_by_side([results_ref[:, z], results_ref[:, z + 1]])).astype(out_ref.dtype)
        for k in range(2):
            out_ref[z + k] = rows[:, k * lanes : (k + 1) * lanes]


def call(body, out_shape, in_specs, scratch=(), flops=0):
    outs = jax.tree.map(lambda _: VMEM, out_shape)
    return pl.pallas_call(
        body,
        out_shape=out_shape,
        in_specs=list(in_specs),
        out_specs=outs,
        scratch_shapes=list(scratch),
        cost_estimate=pl.CostEstimate(flops=flops, transcendentals=0, bytes_accessed=flops // 400),
        compiler_params=pltpu.CompilerParams(vmem_limit_bytes=16 * 1024 * 1024),
    )


def shards(tokens, route_ids, gate_weights, w_gate, w_up, w_down):
    experts = lax.axis_size("expert")
    chips = lax.axis_size(Z)
    token_count, lanes = tokens.shape
    slots = experts * CAP
    _, width_in, width = w_gate.shape
    bf16, f32 = jnp.bfloat16, jnp.float32
    shape = jax.ShapeDtypeStruct

    routes, weights = route_ids.T, gate_weights.T
    place = jnp.stack([lax.axis_index("core"), lax.axis_index("z_1")]).astype(jnp.int32)
    tokens, place = lax.optimization_barrier((tokens, place))

    swap = functools.partial(lax.ppermute, axis_name="core", perm=[(0, 1), (1, 0)])
    exchange = functools.partial(lax.all_to_all, split_axis=0, concat_axis=0, tiled=True)

    picked = call(dispatch_body, shape((experts, CAP + MARK_ROWS, lanes), bf16), (VMEM, VMEM))(routes, tokens)
    slices = exchange(picked.astype(jnp.float16), "expert")
    own = lax.all_gather(slices, Z, axis=0, tiled=False).astype(bf16)
    other = swap(own)

    gate_rows, up_rows, down_rows = w_gate[0].T, w_up[0].T, w_down[0]
    up_rows = pltpu.with_memory_space_constraint(up_rows, pltpu.HBM)
    up_flops = 2 * slots * width * width_in
    acc = shape((slots, width), f32)
    gate_half, up_half, up_here, combine_table = call(
        first_half_body,
        (acc, acc, shape((width, width_in), bf16), shape((token_count, slots), bf16)),
        (SMEM, VMEM, VMEM, VMEM, VMEM, HBM),
        [pltpu.SemaphoreType.DMA((CHUNKS,))],
        flops=up_flops,
    )(place, own, routes, weights, gate_rows, up_rows)
    of_parity = chips // PARITIES
    half = shape((experts, of_parity, CAP, lanes), bf16)
    quarter = shape((experts, of_parity // 2, CAP, lanes), bf16)
    wide = shape(half.shape, f32)

    def down(out, **which):
        body = functools.partial(down_body, **which)
        return call(body, out, (SMEM, VMEM, VMEM), flops=up_flops // 4)(place, hidden, down_rows)

    hidden, theirs_away = call(
        second_half_body,
        (shape((slots, width), bf16), half),
        (SMEM, VMEM, VMEM, VMEM, VMEM, VMEM, VMEM),
        flops=up_flops * 5 // 4,
    )(place, other, gate_half, up_half, gate_rows, up_here, down_rows)
    arrived_away = swap(theirs_away)
    mine_away = down(wide, own_core=True, own_parity=False)
    right, left = call(outgoing_body, (quarter, quarter), (VMEM, VMEM))(mine_away, arrived_away)
    low = lax.ppermute(right, Z, [(z, (z + 1) % chips) for z in range(chips)])
    high = lax.ppermute(left, Z, [(z, (z - 1) % chips) for z in range(chips)])
    arrived = swap(down(half, own_core=False, own_parity=True))
    mine = down(wide, own_core=True, own_parity=True)
    paired = call(pair_body, half, (VMEM,) * 4)(mine, arrived, low, high)

    results = exchange(paired, "expert")
    blended = call(combine_body, shape((of_parity, token_count, lanes), bf16), (VMEM, VMEM))(combine_table, results)
    pieces = exchange(blended, "z_0")
    return pieces.astype(f32).sum(axis=0).astype(bf16)


def solution(mesh):
    groups, experts, etp = (mesh.shape[name] for name in ("groups", "expert", "etp"))
    finer = Mesh(
        mesh.devices.reshape(groups, experts, etp // (CORES * PARITIES), PARITIES, CORES),
        ("groups", "expert", *ETP),
    )
    placed = (
        P(("groups", "expert"), ETP),
        P(("groups", "expert"), None),
        P(("groups", "expert"), None),
        P("expert", None, ETP),
        P("expert", None, ETP),
        P("expert", ETP, None),
    )
    return jax.shard_map(
        shards, mesh=finer, in_specs=placed, out_specs=P(("groups", "expert"), ETP), check_vma=False
    )
```

```python
import functools

import jax
import jax.numpy as jnp
from jax import lax
from jax.experimental import pallas as pl
from jax.experimental.pallas import tpu as pltpu
from jax.sharding import Mesh
from jax.sharding import PartitionSpec as P


CAP = 96
CORES = 2
Z = ("z_0", "z_1")
ETP = (*Z, "core")
LANES = 128
CHUNKS = 4
TOP = 12
LEVELS = 14
MARK_ROWS = 8
PARITIES = 2

HBM = pl.BlockSpec(memory_space=pltpu.HBM)
VMEM = pl.BlockSpec(memory_space=pltpu.VMEM)
SMEM = pl.BlockSpec(memory_space=pltpu.SMEM)


def dot32(a, b):
    return jnp.dot(a, b, preferred_element_type=jnp.float32)


def side_by_side(tiles):
    return jnp.concatenate([tile.reshape(-1, LANES) for tile in tiles], axis=1)


def slot_table(routes_ref, cap, experts, weight_of):
    tokens = routes_ref.shape[1]
    rows = -(-experts // 8) * 8
    expert = lax.broadcasted_iota(jnp.int32, (rows, tokens), 0)
    hit = (routes_ref[0:1, :] == expert) | (routes_ref[1:2, :] == expert)
    square = (tokens, tokens)
    earlier = lax.broadcasted_iota(jnp.int32, square, 0) < lax.broadcasted_iota(jnp.int32, square, 1)
    ones = [jnp.where(mask, 1.0, 0.0).astype(jnp.bfloat16) for mask in (hit, earlier)]
    slot = jnp.where(hit, dot32(*ones), -1.0).astype(jnp.int32)
    number = lax.broadcasted_iota(jnp.int32, (cap, tokens), 0)
    parts = [jnp.where(slot[e : e + 1, :] == number, weight_of(e), 0.0) for e in range(experts)]
    return jnp.concatenate(parts, axis=0).astype(jnp.bfloat16)


def dispatch_body(routes_in, tokens_in, out_ref, routes_ref, tokens_ref, sems):
    experts, rows, lanes = out_ref.shape
    pairs = ((routes_in, routes_ref), (tokens_in, tokens_ref))
    copies = [pltpu.make_async_copy(source, target, sems.at[i]) for i, (source, target) in enumerate(pairs)]
    for copy in copies:
        copy.start()
    for copy in copies:
        copy.wait()
    tokens = tokens_ref[...]
    largest = jnp.max(jnp.abs(tokens.astype(jnp.float32)))
    scale, mark = jnp.float32(2.0**TOP), jnp.float32(1.0)
    for level in range(1, LEVELS):
        lower = largest < 2.0 ** (15 - TOP - 8 * level)
        scale = jnp.where(lower, 2.0 ** (TOP + 8 * level), scale)
        mark = jnp.where(lower, 2.0**-level, mark)
    picked = dot32(slot_table(routes_ref, CAP, experts, lambda e: 1.0), tokens) * scale
    out_ref[:, :CAP] = picked.astype(out_ref.dtype).reshape(experts, CAP, lanes)
    out_ref[:, CAP:] = jnp.full((experts, rows - CAP, lanes), mark, jnp.float32).astype(out_ref.dtype)


def unscaled(tile_ref, z):
    mark = tile_ref[z, :, CAP : CAP + 1].astype(jnp.float32)
    for _ in range(3):
        mark = mark * mark
    return tile_ref[z, :, :CAP] * (mark * 2.0**-TOP).astype(tile_ref.dtype)


def column_copies(w_ref, buf, sems):
    step = w_ref.shape[1] // CHUNKS
    spans = [pl.ds(k * step, step) for k in range(CHUNKS)]
    return [pltpu.make_async_copy(w_ref.at[:, span], buf.at[:, span], sems.at[i]) for i, span in enumerate(spans)]


def core_columns(ref, core, chips):
    return side_by_side([ref[:, pl.ds(pl.multiple_of((z * CORES + core) * LANES, LANES), LANES)] for z in chips])


def down_into(hidden, core, parity, wd_ref, out_ref):
    blocks, count, cap, lanes = out_ref.shape
    step = 4
    for k in range(0, count, step):
        chips = [PARITIES * z + parity for z in range(k, k + step)]
        part = dot32(hidden, core_columns(wd_ref, core, chips)).astype(out_ref.dtype)
        for z in range(step):
            out_ref[:, k + z] = part[:, z * lanes : (z + 1) * lanes].reshape(blocks, cap, lanes)


def up_body(place_ref, x_ref, wg_ref, wu_ref, wd_ref, hidden_ref, out_ref, d_here, u_buf, x_buf, sems):
    core, parity = place_ref[0], place_ref[1]
    ups = column_copies(wu_ref, u_buf, sems.at[0])
    downs = column_copies(wd_ref, d_here, sems.at[1])
    for copy in ups + downs:
        copy.start()
    step = x_ref.shape[0] // CHUNKS
    spans = [slice(k * step * LANES, (k + 1) * step * LANES) for k in range(CHUNKS)]

    def part(x, w):
        return lax.dot_general(x, w, (((1,), (1,)), ((), ())), preferred_element_type=jnp.float32)

    gate = up = None
    for k, span in enumerate(spans):
        x = side_by_side([unscaled(x_ref, z) for z in range(k * step, (k + 1) * step)])
        x_buf[:, span] = x
        gate = part(x, wg_ref[:, span]) if k == 0 else gate + part(x, wg_ref[:, span])
    for k, span in enumerate(spans):
        ups[k].wait()
        more = part(x_buf[:, span], u_buf[:, span])
        up = more if k == 0 else up + more
    hidden = (gate / (1.0 + jnp.exp(-gate)) * up).astype(hidden_ref.dtype)
    hidden_ref[...] = hidden
    for copy in downs:
        copy.wait()
    down_into(hidden, 1 - core, 1 - parity, d_here, out_ref)


def down_body(place_ref, hidden_ref, wd_ref, out_ref, *, own_core, own_parity):
    core, parity = place_ref[0], place_ref[1]
    down_into(
        hidden_ref[...], core if own_core else 1 - core, parity if own_parity else 1 - parity, wd_ref, out_ref
    )


def last_down_body(place_ref, hidden_ref, wd_ref, routes_ref, weights_ref, out_ref, table_ref):
    def weight_of(e):
        return sum(jnp.where(routes_ref[k : k + 1, :] == e, weights_ref[k : k + 1, :], 0.0) for k in range(2))

    table_ref[...] = slot_table(routes_ref, out_ref.shape[2], out_ref.shape[0], weight_of).T
    down_into(hidden_ref[...], place_ref[0], place_ref[1], wd_ref, out_ref)


def outgoing_body(mine_ref, arrived_ref, right_ref, left_ref):
    half = right_ref.shape[1]
    for part, ref in enumerate((right_ref, left_ref)):
        chips = pl.ds(part * half, half)
        ref[...] = (mine_ref[:, chips] + arrived_ref[:, chips].astype(jnp.float32)).astype(ref.dtype)


def pair_body(mine_ref, arrived_ref, low_ref, high_ref, out_ref):
    half = low_ref.shape[1]
    for part, ref in enumerate((low_ref, high_ref)):
        chips = pl.ds(part * half, half)
        total = mine_ref[:, chips] + arrived_ref[:, chips].astype(jnp.float32) + ref[...].astype(jnp.float32)
        out_ref[:, chips] = total.astype(out_ref.dtype)


def combine_body(table_ref, results_ref, out_ref):
    chips, _, lanes = out_ref.shape
    table = table_ref[...]
    for z in range(0, chips, 2):
        rows = dot32(table, side_by_side([results_ref[:, z], results_ref[:, z + 1]])).astype(out_ref.dtype)
        for k in range(2):
            out_ref[z + k] = rows[:, k * lanes : (k + 1) * lanes]


def call(body, out_shape, in_specs, scratch=(), flops=0):
    outs = jax.tree.map(lambda _: VMEM, out_shape)
    return pl.pallas_call(
        body,
        out_shape=out_shape,
        in_specs=list(in_specs),
        out_specs=outs,
        scratch_shapes=list(scratch),
        cost_estimate=pl.CostEstimate(flops=flops, transcendentals=0, bytes_accessed=flops // 400),
        compiler_params=pltpu.CompilerParams(vmem_limit_bytes=16 * 1024 * 1024),
    )


def layer(tokens, route_ids, gate_weights, w_gate, w_up, w_down):
    experts = lax.axis_size("expert")
    chips = lax.axis_size(Z)
    token_count, lanes = tokens.shape
    slots = experts * CAP
    _, width_in, width = w_gate.shape
    bf16, f32 = jnp.bfloat16, jnp.float32
    shape = jax.ShapeDtypeStruct

    routes, weights = route_ids.T, gate_weights.T
    place = jnp.stack([lax.axis_index("core"), lax.axis_index("z_1")]).astype(jnp.int32)
    tokens, place = lax.optimization_barrier((tokens, place))

    swap = functools.partial(lax.ppermute, axis_name="core", perm=[(0, 1), (1, 0)])
    exchange = functools.partial(lax.all_to_all, split_axis=0, concat_axis=0, tiled=True)

    first_routes, first_tokens, up_rows, down_rows = (
        pltpu.with_memory_space_constraint(v, pltpu.HBM) for v in (routes, tokens, w_up[0].T, w_down[0])
    )
    picked = call(
        dispatch_body,
        shape((experts, CAP + MARK_ROWS, lanes), bf16),
        (HBM, HBM),
        [pltpu.VMEM(routes.shape, routes.dtype), pltpu.VMEM(tokens.shape, tokens.dtype), pltpu.SemaphoreType.DMA((2,))],
    )(first_routes, first_tokens)
    slices = exchange(picked.astype(jnp.float16), "expert")
    rows = lax.all_gather(slices, ETP, axis=0, tiled=False).astype(bf16)

    of_parity = chips // PARITIES
    half = shape((experts, of_parity, CAP, lanes), bf16)
    quarter = shape((experts, of_parity // 2, CAP, lanes), bf16)
    wide = shape(half.shape, f32)
    held = shape((width, width_in), bf16)
    down_flops = slots * width * width_in // 2

    hidden, theirs_away, down_here = call(
        up_body,
        (shape((slots, width), bf16), half, held),
        (SMEM, VMEM, VMEM, HBM, HBM),
        [pltpu.VMEM(held.shape, bf16), pltpu.VMEM((slots, width_in), bf16), pltpu.SemaphoreType.DMA((2, CHUNKS))],
        flops=9 * down_flops,
    )(place, rows, w_gate[0].T, up_rows, down_rows)
    arrived_away = swap(theirs_away)
    mine_away = call(
        functools.partial(down_body, own_core=True, own_parity=False), wide, (SMEM, VMEM, VMEM), flops=down_flops
    )(place, hidden, down_here)
    right, left = call(outgoing_body, (quarter, quarter), (VMEM, VMEM))(mine_away, arrived_away)
    low = lax.ppermute(right, Z, [(z, (z + 1) % chips) for z in range(chips)])
    high = lax.ppermute(left, Z, [(z, (z - 1) % chips) for z in range(chips)])
    theirs = call(
        functools.partial(down_body, own_core=False, own_parity=True), half, (SMEM, VMEM, VMEM), flops=down_flops
    )(place, hidden, down_here)
    arrived = swap(theirs)
    mine, combine_table = call(
        last_down_body, (wide, shape((token_count, slots), bf16)), (SMEM,) + (VMEM,) * 4, flops=down_flops
    )(place, hidden, down_here, routes, weights)
    paired = call(pair_body, half, (VMEM,) * 4)(mine, arrived, low, high)

    results = exchange(paired, "expert")
    blended = call(combine_body, shape((of_parity, token_count, lanes), bf16), (VMEM, VMEM))(combine_table, results)
    pieces = exchange(blended, "z_0")
    return pieces.astype(f32).sum(axis=0).astype(bf16)


def solution(mesh):
    groups, experts, etp = (mesh.shape[name] for name in ("groups", "expert", "etp"))
    finer = Mesh(
        mesh.devices.reshape(groups, experts, etp // (CORES * PARITIES), PARITIES, CORES),
        ("groups", "expert", *ETP),
    )
    placed = (
        P(("groups", "expert"), ETP),
        P(("groups", "expert"), None),
        P(("groups", "expert"), None),
        P("expert", None, ETP),
        P("expert", None, ETP),
        P("expert", ETP, None),
    )
    return jax.shard_map(layer, mesh=finer, in_specs=placed, out_specs=P(("groups", "expert"), ETP), check_vma=False)
```

```python
import functools

import jax
import jax.numpy as jnp
from jax import lax
from jax.experimental import pallas as pl
from jax.experimental.pallas import tpu as pltpu
from jax.sharding import Mesh
from jax.sharding import PartitionSpec as P


CAP = 96
CORES = 2
Z = ("z_0", "z_1")
ETP = (*Z, "core")
LANES = 128
CHUNKS = 4
PARITIES = 2

HBM = pl.BlockSpec(memory_space=pltpu.HBM)
VMEM = pl.BlockSpec(memory_space=pltpu.VMEM)
SMEM = pl.BlockSpec(memory_space=pltpu.SMEM)


def dot32(a, b):
    return jnp.dot(a, b, preferred_element_type=jnp.float32)


def side_by_side(tiles):
    return jnp.concatenate([tile.reshape(-1, LANES) for tile in tiles], axis=1)


def slot_table(routes_ref, cap, experts, weight_of):
    tokens = routes_ref.shape[1]
    rows = -(-experts // 8) * 8
    expert = lax.broadcasted_iota(jnp.int32, (rows, tokens), 0)
    hit = (routes_ref[0:1, :] == expert) | (routes_ref[1:2, :] == expert)
    square = (tokens, tokens)
    earlier = lax.broadcasted_iota(jnp.int32, square, 0) < lax.broadcasted_iota(jnp.int32, square, 1)
    ones = [jnp.where(mask, 1.0, 0.0).astype(jnp.bfloat16) for mask in (hit, earlier)]
    slot = jnp.where(hit, dot32(*ones), -1.0).astype(jnp.int32)
    number = lax.broadcasted_iota(jnp.int32, (cap, tokens), 0)
    parts = [jnp.where(slot[e : e + 1, :] == number, weight_of(e), 0.0) for e in range(experts)]
    return jnp.concatenate(parts, axis=0).astype(jnp.bfloat16)


def dispatch_body(routes_ref, tokens_ref, out_ref):
    experts, chips, cap, lanes = out_ref.shape
    table = slot_table(routes_ref, cap, experts, lambda e: 1.0)
    for z in range(0, chips, 2):
        rows = dot32(table, side_by_side([tokens_ref[z], tokens_ref[z + 1]])).astype(out_ref.dtype)
        for k in range(2):
            out_ref[:, z + k] = rows[:, k * lanes : (k + 1) * lanes].reshape(experts, cap, lanes)


def column_copies(w_ref, buf, sems):
    step = w_ref.shape[1] // CHUNKS
    spans = [pl.ds(k * step, step) for k in range(CHUNKS)]
    return [pltpu.make_async_copy(w_ref.at[:, span], buf.at[:, span], sems.at[i]) for i, span in enumerate(spans)]


def core_columns(ref, core, chips):
    return side_by_side([ref[:, pl.ds(pl.multiple_of((z * CORES + core) * LANES, LANES), LANES)] for z in chips])


def down_into(hidden, core, parity, wd_ref, out_ref):
    blocks, count, cap, lanes = out_ref.shape
    step = 4
    for k in range(0, count, step):
        chips = [PARITIES * z + parity for z in range(k, k + step)]
        part = dot32(hidden, core_columns(wd_ref, core, chips)).astype(out_ref.dtype)
        for z in range(step):
            out_ref[:, k + z] = part[:, z * lanes : (z + 1) * lanes].reshape(blocks, cap, lanes)


def up_partial(core, x_ref, w_ref, copies=None):
    step = x_ref.shape[1] // CHUNKS
    total = None
    for k in range(CHUNKS):
        chips = range(k * step, (k + 1) * step)
        if copies is not None:
            copies[k].wait()
        part = lax.dot_general(
            side_by_side([x_ref[:, z] for z in chips]),
            core_columns(w_ref, core, chips),
            (((1,), (1,)), ((), ())),
            preferred_element_type=jnp.float32,
        )
        total = part if k == 0 else total + part
    return total


def first_half_body(place_ref, x_ref, wg_ref, wu_ref, gate_ref, up_ref, u_here, sems):
    copies = column_copies(wu_ref, u_here, sems)
    for copy in copies:
        copy.start()
    gate_ref[...] = up_partial(place_ref[0], x_ref, wg_ref)
    up_ref[...] = up_partial(place_ref[0], x_ref, u_here, copies)


def second_half_body(place_ref, x_ref, gate_ref, up_ref, wg_ref, wu_ref, wd_ref, hidden_ref, out_ref):
    core, parity = place_ref[0], place_ref[1]
    gate = up_partial(1 - core, x_ref, wg_ref) + gate_ref[...]
    up = up_partial(1 - core, x_ref, wu_ref) + up_ref[...]
    hidden = (gate / (1.0 + jnp.exp(-gate)) * up).astype(hidden_ref.dtype)
    hidden_ref[...] = hidden
    down_into(hidden, 1 - core, 1 - parity, wd_ref, out_ref)


def down_body(place_ref, hidden_ref, wd_ref, out_ref, *, own_core, own_parity):
    core, parity = place_ref[0], place_ref[1]
    down_into(
        hidden_ref[...], core if own_core else 1 - core, parity if own_parity else 1 - parity, wd_ref, out_ref
    )


def last_down_body(place_ref, hidden_ref, wd_ref, routes_ref, weights_ref, out_ref, table_ref):
    def weight_of(e):
        return sum(jnp.where(routes_ref[k : k + 1, :] == e, weights_ref[k : k + 1, :], 0.0) for k in range(2))

    table_ref[...] = slot_table(routes_ref, out_ref.shape[2], out_ref.shape[0], weight_of).T
    down_into(hidden_ref[...], place_ref[0], place_ref[1], wd_ref, out_ref)


def outgoing_body(mine_ref, arrived_ref, right_ref, left_ref):
    half = right_ref.shape[1]
    for part, ref in enumerate((right_ref, left_ref)):
        chips = pl.ds(part * half, half)
        ref[...] = (mine_ref[:, chips] + arrived_ref[:, chips].astype(jnp.float32)).astype(ref.dtype)


def pair_body(mine_ref, arrived_ref, low_ref, high_ref, out_ref):
    half = low_ref.shape[1]
    for part, ref in enumerate((low_ref, high_ref)):
        chips = pl.ds(part * half, half)
        total = mine_ref[:, chips] + arrived_ref[:, chips].astype(jnp.float32) + ref[...].astype(jnp.float32)
        out_ref[:, chips] = total.astype(out_ref.dtype)


def combine_body(table_ref, results_ref, out_ref):
    chips, _, lanes = out_ref.shape
    table = table_ref[...]
    for z in range(0, chips, 2):
        rows = dot32(table, side_by_side([results_ref[:, z], results_ref[:, z + 1]])).astype(out_ref.dtype)
        for k in range(2):
            out_ref[z + k] = rows[:, k * lanes : (k + 1) * lanes]


def call(body, out_shape, in_specs, scratch=(), flops=0):
    outs = jax.tree.map(lambda _: VMEM, out_shape)
    return pl.pallas_call(
        body,
        out_shape=out_shape,
        in_specs=list(in_specs),
        out_specs=outs,
        scratch_shapes=list(scratch),
        cost_estimate=pl.CostEstimate(flops=flops, transcendentals=0, bytes_accessed=flops // 400),
        compiler_params=pltpu.CompilerParams(vmem_limit_bytes=16 * 1024 * 1024),
    )


def layer(tokens, route_ids, gate_weights, w_gate, w_up, w_down):
    experts = lax.axis_size("expert")
    chips = lax.axis_size(Z)
    token_count, lanes = tokens.shape
    slots = experts * CAP
    _, width_in, width = w_gate.shape
    bf16, f32 = jnp.bfloat16, jnp.float32
    shape = jax.ShapeDtypeStruct

    routes, weights = route_ids.T, gate_weights.T
    place = jnp.stack([lax.axis_index("core"), lax.axis_index("z_1")]).astype(jnp.int32)
    tokens, place = lax.optimization_barrier((tokens, place))

    swap = functools.partial(lax.ppermute, axis_name="core", perm=[(0, 1), (1, 0)])
    exchange = functools.partial(lax.all_to_all, split_axis=0, concat_axis=0, tiled=True)

    gathered = lax.all_gather(tokens, Z, axis=0, tiled=False)
    picked = call(
        dispatch_body, shape((experts, chips, CAP, lanes), bf16), (VMEM, VMEM), flops=2 * slots * token_count * chips * lanes
    )(routes, gathered)
    own = exchange(picked, "expert")
    other = swap(own)

    of_parity = chips // PARITIES
    half = shape((experts, of_parity, CAP, lanes), bf16)
    quarter = shape((experts, of_parity // 2, CAP, lanes), bf16)
    wide = shape(half.shape, f32)
    acc = shape((slots, width), f32)
    held = shape((width, width_in), bf16)
    down_flops = slots * width * width_in // 2
    gate_rows, up_rows, down_rows = w_gate[0].T, w_up[0].T, w_down[0]
    up_rows = pltpu.with_memory_space_constraint(up_rows, pltpu.HBM)

    gate_half, up_half, up_here = call(
        first_half_body,
        (acc, acc, held),
        (SMEM, VMEM, VMEM, HBM),
        [pltpu.SemaphoreType.DMA((CHUNKS,))],
        flops=4 * down_flops,
    )(place, own, gate_rows, up_rows)
    hidden, theirs_away = call(
        second_half_body, (shape((slots, width), bf16), half), (SMEM,) + (VMEM,) * 6, flops=5 * down_flops
    )(place, other, gate_half, up_half, gate_rows, up_here, down_rows)
    arrived_away = swap(theirs_away)
    mine_away = call(
        functools.partial(down_body, own_core=True, own_parity=False), wide, (SMEM, VMEM, VMEM), flops=down_flops
    )(place, hidden, down_rows)
    right, left = call(outgoing_body, (quarter, quarter), (VMEM, VMEM))(mine_away, arrived_away)
    low = lax.ppermute(right, Z, [(z, (z + 1) % chips) for z in range(chips)])
    high = lax.ppermute(left, Z, [(z, (z - 1) % chips) for z in range(chips)])
    theirs = call(
        functools.partial(down_body, own_core=False, own_parity=True), half, (SMEM, VMEM, VMEM), flops=down_flops
    )(place, hidden, down_rows)
    arrived = swap(theirs)
    mine, combine_table = call(
        last_down_body, (wide, shape((token_count, slots), bf16)), (SMEM,) + (VMEM,) * 4, flops=down_flops
    )(place, hidden, down_rows, routes, weights)
    paired = call(pair_body, half, (VMEM,) * 4)(mine, arrived, low, high)

    results = exchange(paired, "expert")
    blended = call(combine_body, shape((of_parity, token_count, lanes), bf16), (VMEM, VMEM))(combine_table, results)
    pieces = exchange(blended, "z_0")
    return pieces.astype(f32).sum(axis=0).astype(bf16)


def solution(mesh):
    groups, experts, etp = (mesh.shape[name] for name in ("groups", "expert", "etp"))
    finer = Mesh(
        mesh.devices.reshape(groups, experts, etp // (CORES * PARITIES), PARITIES, CORES),
        ("groups", "expert", *ETP),
    )
    placed = (
        P(("groups", "expert"), ETP),
        P(("groups", "expert"), None),
        P(("groups", "expert"), None),
        P("expert", None, ETP),
        P("expert", None, ETP),
        P("expert", ETP, None),
    )
    return jax.shard_map(layer, mesh=finer, in_specs=placed, out_specs=P(("groups", "expert"), ETP), check_vma=False)
```

```python
import functools

import jax
import jax.numpy as jnp
from jax import lax
from jax.experimental import pallas as pl
from jax.experimental.pallas import tpu as pltpu
from jax.sharding import Mesh
from jax.sharding import PartitionSpec as P


CAP = 96
CORES = 2
Z = ("z_0", "z_1")
ETP = (*Z, "core")
LANES = 128
CHUNKS = 4
TOP = 12
LEVELS = 14
MARK_ROWS = 8
PARITIES = 2

HBM = pl.BlockSpec(memory_space=pltpu.HBM)
VMEM = pl.BlockSpec(memory_space=pltpu.VMEM)
SMEM = pl.BlockSpec(memory_space=pltpu.SMEM)


def dot32(a, b):
    return jnp.dot(a, b, preferred_element_type=jnp.float32)


def side_by_side(tiles):
    return jnp.concatenate([tile.reshape(-1, LANES) for tile in tiles], axis=1)


def slot_table(routes_ref, cap, experts, weight_of):
    tokens = routes_ref.shape[1]
    rows = -(-experts // 8) * 8
    expert = lax.broadcasted_iota(jnp.int32, (rows, tokens), 0)
    hit = (routes_ref[0:1, :] == expert) | (routes_ref[1:2, :] == expert)
    square = (tokens, tokens)
    earlier = lax.broadcasted_iota(jnp.int32, square, 0) < lax.broadcasted_iota(jnp.int32, square, 1)
    ones = [jnp.where(mask, 1.0, 0.0).astype(jnp.bfloat16) for mask in (hit, earlier)]
    slot = jnp.where(hit, dot32(*ones), -1.0).astype(jnp.int32)
    number = lax.broadcasted_iota(jnp.int32, (cap, tokens), 0)
    parts = [jnp.where(slot[e : e + 1, :] == number, weight_of(e), 0.0) for e in range(experts)]
    return jnp.concatenate(parts, axis=0).astype(jnp.bfloat16)


def dispatch_body(routes_in, tokens_in, out_ref, routes_ref, tokens_ref, sems):
    experts, rows, lanes = out_ref.shape
    pairs = ((routes_in, routes_ref), (tokens_in, tokens_ref))
    copies = [pltpu.make_async_copy(source, target, sems.at[i]) for i, (source, target) in enumerate(pairs)]
    for copy in copies:
        copy.start()
    for copy in copies:
        copy.wait()
    tokens = tokens_ref[...]
    largest = jnp.max(jnp.abs(tokens.astype(jnp.float32)))
    scale, mark = jnp.float32(2.0**TOP), jnp.float32(1.0)
    for level in range(1, LEVELS):
        lower = largest < 2.0 ** (15 - TOP - 8 * level)
        scale = jnp.where(lower, 2.0 ** (TOP + 8 * level), scale)
        mark = jnp.where(lower, 2.0**-level, mark)
    picked = dot32(slot_table(routes_ref, CAP, experts, lambda e: 1.0), tokens) * scale
    out_ref[:, :CAP] = picked.astype(out_ref.dtype).reshape(experts, CAP, lanes)
    out_ref[:, CAP:] = jnp.full((experts, rows - CAP, lanes), mark, jnp.float32).astype(out_ref.dtype)


def unscaled(tile_ref, z):
    mark = tile_ref[z, :, CAP : CAP + 1].astype(jnp.float32)
    for _ in range(3):
        mark = mark * mark
    return tile_ref[z, :, :CAP] * (mark * 2.0**-TOP).astype(tile_ref.dtype)


def column_copies(w_ref, buf, sems):
    step = w_ref.shape[1] // CHUNKS
    spans = [pl.ds(k * step, step) for k in range(CHUNKS)]
    return [pltpu.make_async_copy(w_ref.at[:, span], buf.at[:, span], sems.at[i]) for i, span in enumerate(spans)]


def core_columns(ref, core, chips):
    return side_by_side([ref[:, pl.ds(pl.multiple_of((z * CORES + core) * LANES, LANES), LANES)] for z in chips])


def down_into(hidden, core, parity, wd_ref, out_ref):
    blocks, count, cap, lanes = out_ref.shape
    step = 4
    for k in range(0, count, step):
        chips = [PARITIES * z + parity for z in range(k, k + step)]
        part = dot32(hidden, core_columns(wd_ref, core, chips)).astype(out_ref.dtype)
        for z in range(step):
            out_ref[:, k + z] = part[:, z * lanes : (z + 1) * lanes].reshape(blocks, cap, lanes)


def up_partial(core, x_ref, w_ref, copies=None):
    step = x_ref.shape[0] // CHUNKS
    total = None
    for k in range(CHUNKS):
        chips = range(k * step, (k + 1) * step)
        x = side_by_side([unscaled(x_ref, z) for z in chips])
        if copies is not None:
            copies[k].wait()
        part = lax.dot_general(
            x, core_columns(w_ref, core, chips), (((1,), (1,)), ((), ())), preferred_element_type=jnp.float32
        )
        total = part if k == 0 else total + part
    return total


def first_half_body(place_ref, x_ref, wg_ref, wu_ref, gate_ref, up_ref, u_here, sems):
    copies = column_copies(wu_ref, u_here, sems)
    for copy in copies:
        copy.start()
    gate_ref[...] = up_partial(place_ref[0], x_ref, wg_ref)
    up_ref[...] = up_partial(place_ref[0], x_ref, u_here, copies)


def second_half_body(place_ref, x_ref, gate_ref, up_ref, wg_ref, wu_ref, wd_ref, hidden_ref, out_ref):
    core, parity = place_ref[0], place_ref[1]
    gate = up_partial(1 - core, x_ref, wg_ref) + gate_ref[...]
    up = up_partial(1 - core, x_ref, wu_ref) + up_ref[...]
    hidden = (gate / (1.0 + jnp.exp(-gate)) * up).astype(hidden_ref.dtype)
    hidden_ref[...] = hidden
    down_into(hidden, 1 - core, 1 - parity, wd_ref, out_ref)


def down_body(place_ref, hidden_ref, wd_ref, out_ref, *, own_core, own_parity):
    core, parity = place_ref[0], place_ref[1]
    down_into(
        hidden_ref[...], core if own_core else 1 - core, parity if own_parity else 1 - parity, wd_ref, out_ref
    )


def last_down_body(place_ref, hidden_ref, wd_ref, routes_ref, weights_ref, out_ref, table_ref):
    def weight_of(e):
        return sum(jnp.where(routes_ref[k : k + 1, :] == e, weights_ref[k : k + 1, :], 0.0) for k in range(2))

    table_ref[...] = slot_table(routes_ref, out_ref.shape[2], out_ref.shape[0], weight_of).T
    down_into(hidden_ref[...], place_ref[0], place_ref[1], wd_ref, out_ref)


def outgoing_body(mine_ref, arrived_ref, right_ref, left_ref):
    half = right_ref.shape[1]
    for part, ref in enumerate((right_ref, left_ref)):
        chips = pl.ds(part * half, half)
        ref[...] = (mine_ref[:, chips] + arrived_ref[:, chips].astype(jnp.float32)).astype(ref.dtype)


def pair_body(mine_ref, arrived_ref, low_ref, high_ref, out_ref):
    half = low_ref.shape[1]
    for part, ref in enumerate((low_ref, high_ref)):
        chips = pl.ds(part * half, half)
        total = mine_ref[:, chips] + arrived_ref[:, chips].astype(jnp.float32) + ref[...].astype(jnp.float32)
        out_ref[:, chips] = total.astype(out_ref.dtype)


def combine_body(table_ref, results_ref, out_ref):
    chips, _, lanes = out_ref.shape
    table = table_ref[...]
    for z in range(0, chips, 2):
        rows = dot32(table, side_by_side([results_ref[:, z], results_ref[:, z + 1]])).astype(out_ref.dtype)
        for k in range(2):
            out_ref[z + k] = rows[:, k * lanes : (k + 1) * lanes]


def call(body, out_shape, in_specs, scratch=(), flops=0):
    outs = jax.tree.map(lambda _: VMEM, out_shape)
    return pl.pallas_call(
        body,
        out_shape=out_shape,
        in_specs=list(in_specs),
        out_specs=outs,
        scratch_shapes=list(scratch),
        cost_estimate=pl.CostEstimate(flops=flops, transcendentals=0, bytes_accessed=flops // 400),
        compiler_params=pltpu.CompilerParams(vmem_limit_bytes=16 * 1024 * 1024),
    )


def layer(tokens, route_ids, gate_weights, w_gate, w_up, w_down):
    experts = lax.axis_size("expert")
    chips = lax.axis_size(Z)
    token_count, lanes = tokens.shape
    slots = experts * CAP
    _, width_in, width = w_gate.shape
    bf16, f32 = jnp.bfloat16, jnp.float32
    shape = jax.ShapeDtypeStruct

    routes, weights = route_ids.T, gate_weights.T
    place = jnp.stack([lax.axis_index("core"), lax.axis_index("z_1")]).astype(jnp.int32)
    tokens, place = lax.optimization_barrier((tokens, place))

    swap = functools.partial(lax.ppermute, axis_name="core", perm=[(0, 1), (1, 0)])
    exchange = functools.partial(lax.all_to_all, split_axis=0, concat_axis=0, tiled=True)

    first_routes, first_tokens, up_rows = (
        pltpu.with_memory_space_constraint(v, pltpu.HBM) for v in (routes, tokens, w_up[0].T)
    )
    picked = call(
        dispatch_body,
        shape((experts, CAP + MARK_ROWS, lanes), bf16),
        (HBM, HBM),
        [pltpu.VMEM(routes.shape, routes.dtype), pltpu.VMEM(tokens.shape, tokens.dtype), pltpu.SemaphoreType.DMA((2,))],
    )(first_routes, first_tokens)
    slices = exchange(picked.astype(jnp.float16), "expert")
    own = lax.all_gather(slices.reshape(-1, lanes), Z, axis=0, tiled=True)
    own = own.reshape(chips, *slices.shape).astype(bf16)
    other = swap(own)

    of_parity = chips // PARITIES
    half = shape((experts, of_parity, CAP, lanes), bf16)
    quarter = shape((experts, of_parity // 2, CAP, lanes), bf16)
    wide = shape(half.shape, f32)
    acc = shape((slots, width), f32)
    held = shape((width, width_in), bf16)
    gate_rows, down_rows = w_gate[0].T, w_down[0]
    down_flops = slots * width * width_in // 2

    gate_half, up_half, up_here = call(
        first_half_body,
        (acc, acc, held),
        (SMEM, VMEM, VMEM, HBM),
        [pltpu.SemaphoreType.DMA((CHUNKS,))],
        flops=4 * down_flops,
    )(place, own, gate_rows, up_rows)
    hidden, theirs_away = call(
        second_half_body, (shape((slots, width), bf16), half), (SMEM,) + (VMEM,) * 6, flops=5 * down_flops
    )(place, other, gate_half, up_half, gate_rows, up_here, down_rows)
    arrived_away = swap(theirs_away)
    mine_away = call(
        functools.partial(down_body, own_core=True, own_parity=False), wide, (SMEM, VMEM, VMEM), flops=down_flops
    )(place, hidden, down_rows)
    right, left = call(outgoing_body, (quarter, quarter), (VMEM, VMEM))(mine_away, arrived_away)
    low = lax.ppermute(right, Z, [(z, (z + 1) % chips) for z in range(chips)])
    high = lax.ppermute(left, Z, [(z, (z - 1) % chips) for z in range(chips)])
    theirs = call(
        functools.partial(down_body, own_core=False, own_parity=True), half, (SMEM, VMEM, VMEM), flops=down_flops
    )(place, hidden, down_rows)
    arrived = swap(theirs)
    mine, combine_table = call(
        last_down_body, (wide, shape((token_count, slots), bf16)), (SMEM,) + (VMEM,) * 4, flops=down_flops
    )(place, hidden, down_rows, routes, weights)
    paired = call(pair_body, half, (VMEM,) * 4)(mine, arrived, low, high)

    results = exchange(paired, "expert")
    blended = call(combine_body, shape((of_parity, token_count, lanes), bf16), (VMEM, VMEM))(combine_table, results)
    pieces = exchange(blended, "z_0")
    return pieces.astype(f32).sum(axis=0).astype(bf16)


def solution(mesh):
    groups, experts, etp = (mesh.shape[name] for name in ("groups", "expert", "etp"))
    finer = Mesh(
        mesh.devices.reshape(groups, experts, etp // (CORES * PARITIES), PARITIES, CORES),
        ("groups", "expert", *ETP),
    )
    placed = (
        P(("groups", "expert"), ETP),
        P(("groups", "expert"), None),
        P(("groups", "expert"), None),
        P("expert", None, ETP),
        P("expert", None, ETP),
        P("expert", ETP, None),
    )
    return jax.shard_map(layer, mesh=finer, in_specs=placed, out_specs=P(("groups", "expert"), ETP), check_vma=False)
```

```python
import functools

import jax
import jax.numpy as jnp
from jax import lax
from jax.experimental import pallas as pl
from jax.experimental.pallas import tpu as pltpu
from jax.sharding import Mesh
from jax.sharding import PartitionSpec as P


CAP = 96
CORES = 2
Z = ("z_0", "z_1")
ETP = (*Z, "core")
LANES = 128
CHUNKS = 4
TOP = 12
LEVELS = 14
MARK_ROWS = 8
PARITIES = 2

HBM = pl.BlockSpec(memory_space=pltpu.HBM)
VMEM = pl.BlockSpec(memory_space=pltpu.VMEM)
SMEM = pl.BlockSpec(memory_space=pltpu.SMEM)


def dot32(a, b):
    return jnp.dot(a, b, preferred_element_type=jnp.float32)


def side_by_side(tiles):
    return jnp.concatenate([tile.reshape(-1, LANES) for tile in tiles], axis=1)


def slot_table(routes_ref, cap, experts, weight_of):
    tokens = routes_ref.shape[1]
    rows = -(-experts // 8) * 8
    expert = lax.broadcasted_iota(jnp.int32, (rows, tokens), 0)
    hit = (routes_ref[0:1, :] == expert) | (routes_ref[1:2, :] == expert)
    square = (tokens, tokens)
    earlier = lax.broadcasted_iota(jnp.int32, square, 0) < lax.broadcasted_iota(jnp.int32, square, 1)
    ones = [jnp.where(mask, 1.0, 0.0).astype(jnp.bfloat16) for mask in (hit, earlier)]
    slot = jnp.where(hit, dot32(*ones), -1.0).astype(jnp.int32)
    number = lax.broadcasted_iota(jnp.int32, (cap, tokens), 0)
    parts = [jnp.where(slot[e : e + 1, :] == number, weight_of(e), 0.0) for e in range(experts)]
    return jnp.concatenate(parts, axis=0).astype(jnp.bfloat16)


def dispatch_body(routes_in, tokens_in, out_ref, routes_ref, tokens_ref, sems):
    experts, cap, lanes = out_ref.shape
    pairs = ((routes_in, routes_ref), (tokens_in, tokens_ref))
    copies = [pltpu.make_async_copy(source, target, sems.at[i]) for i, (source, target) in enumerate(pairs)]
    for copy in copies:
        copy.start()
    for copy in copies:
        copy.wait()
    picked = dot32(slot_table(routes_ref, cap, experts, lambda e: 1.0), tokens_ref[...])
    out_ref[...] = picked.astype(out_ref.dtype).reshape(experts, cap, lanes)


def scale_body(slots_ref, out_ref):
    slots = slots_ref[...].astype(jnp.float32)
    count = slots.shape[0]
    largest = jnp.max(jnp.abs(slots))
    scale, mark = jnp.float32(2.0**TOP), jnp.float32(1.0)
    for level in range(1, LEVELS):
        lower = largest < 2.0 ** (15 - TOP - 8 * level)
        scale = jnp.where(lower, 2.0 ** (TOP + 8 * level), scale)
        mark = jnp.where(lower, 2.0**-level, mark)
    out_ref[:count] = (slots * scale).astype(out_ref.dtype)
    out_ref[count:] = jnp.full((MARK_ROWS, LANES), mark, jnp.float32).astype(out_ref.dtype)


def unscaled(tile_ref, z):
    count = tile_ref.shape[1] - MARK_ROWS
    mark = tile_ref[z, count : count + 1].astype(jnp.float32)
    for _ in range(3):
        mark = mark * mark
    return tile_ref[z, :count] * (mark * 2.0**-TOP).astype(tile_ref.dtype)


def column_copies(w_ref, buf, sems):
    step = w_ref.shape[1] // CHUNKS
    spans = [pl.ds(k * step, step) for k in range(CHUNKS)]
    return [pltpu.make_async_copy(w_ref.at[:, span], buf.at[:, span], sems.at[i]) for i, span in enumerate(spans)]


def core_columns(ref, core, chips):
    return side_by_side([ref[:, pl.ds(pl.multiple_of((z * CORES + core) * LANES, LANES), LANES)] for z in chips])


def down_into(hidden, core, parity, wd_ref, out_ref):
    blocks, count, cap, lanes = out_ref.shape
    step = count
    for k in range(0, count, step):
        chips = [PARITIES * z + parity for z in range(k, k + step)]
        part = dot32(hidden, core_columns(wd_ref, core, chips)).astype(out_ref.dtype)
        for z in range(step):
            out_ref[:, k + z] = part[:, z * lanes : (z + 1) * lanes].reshape(blocks, cap, lanes)


def up_partial(core, x_ref, w_ref, copies=None):
    step = x_ref.shape[0] // CHUNKS
    total = None
    for k in range(CHUNKS):
        chips = range(k * step, (k + 1) * step)
        x = side_by_side([unscaled(x_ref, z) for z in chips])
        if copies is not None:
            copies[k].wait()
        part = lax.dot_general(
            x, core_columns(w_ref, core, chips), (((1,), (1,)), ((), ())), preferred_element_type=jnp.float32
        )
        total = part if k == 0 else total + part
    return total


def first_half_body(place_ref, x_ref, wg_ref, wu_ref, gate_ref, up_ref, u_here, sems):
    copies = column_copies(wu_ref, u_here, sems)
    for copy in copies:
        copy.start()
    gate_ref[...] = up_partial(place_ref[0], x_ref, wg_ref)
    up_ref[...] = up_partial(place_ref[0], x_ref, u_here, copies)


def second_half_body(place_ref, x_ref, gate_ref, up_ref, wg_ref, wu_ref, wd_ref, hidden_ref, out_ref):
    core, parity = place_ref[0], place_ref[1]
    gate = up_partial(1 - core, x_ref, wg_ref) + gate_ref[...]
    up = up_partial(1 - core, x_ref, wu_ref) + up_ref[...]
    hidden = (gate / (1.0 + jnp.exp(-gate)) * up).astype(hidden_ref.dtype)
    hidden_ref[...] = hidden
    down_into(hidden, 1 - core, 1 - parity, wd_ref, out_ref)


def down_body(place_ref, hidden_ref, wd_ref, out_ref, *, own_core, own_parity):
    core, parity = place_ref[0], place_ref[1]
    down_into(
        hidden_ref[...], core if own_core else 1 - core, parity if own_parity else 1 - parity, wd_ref, out_ref
    )


def last_down_body(place_ref, hidden_ref, wd_ref, routes_ref, weights_ref, out_ref, table_ref):
    def weight_of(e):
        return sum(jnp.where(routes_ref[k : k + 1, :] == e, weights_ref[k : k + 1, :], 0.0) for k in range(2))

    table_ref[...] = slot_table(routes_ref, out_ref.shape[2], out_ref.shape[0], weight_of).T
    down_into(hidden_ref[...], place_ref[0], place_ref[1], wd_ref, out_ref)


def outgoing_body(mine_ref, arrived_ref, right_ref, left_ref):
    half = right_ref.shape[1]
    for part, ref in enumerate((right_ref, left_ref)):
        chips = pl.ds(part * half, half)
        ref[...] = (mine_ref[:, chips] + arrived_ref[:, chips].astype(jnp.float32)).astype(ref.dtype)


def pair_body(mine_ref, arrived_ref, low_ref, high_ref, out_ref):
    half = low_ref.shape[1]
    for part, ref in enumerate((low_ref, high_ref)):
        chips = pl.ds(part * half, half)
        total = mine_ref[:, chips] + arrived_ref[:, chips].astype(jnp.float32) + ref[...].astype(jnp.float32)
        out_ref[:, chips] = total.astype(out_ref.dtype)


def combine_body(table_ref, results_ref, out_ref):
    chips, _, lanes = out_ref.shape
    table = table_ref[...]
    for z in range(0, chips, 2):
        rows = dot32(table, side_by_side([results_ref[:, z], results_ref[:, z + 1]])).astype(out_ref.dtype)
        for k in range(2):
            out_ref[z + k] = rows[:, k * lanes : (k + 1) * lanes]


def call(body, out_shape, in_specs, scratch=(), flops=0):
    outs = jax.tree.map(lambda _: VMEM, out_shape)
    return pl.pallas_call(
        body,
        out_shape=out_shape,
        in_specs=list(in_specs),
        out_specs=outs,
        scratch_shapes=list(scratch),
        cost_estimate=pl.CostEstimate(flops=flops, transcendentals=0, bytes_accessed=flops // 400),
        compiler_params=pltpu.CompilerParams(vmem_limit_bytes=16 * 1024 * 1024),
    )


def layer(tokens, route_ids, gate_weights, w_gate, w_up, w_down):
    experts = lax.axis_size("expert")
    chips = lax.axis_size(Z)
    token_count, lanes = tokens.shape
    slots = experts * CAP
    _, width_in, width = w_gate.shape
    bf16, f32 = jnp.bfloat16, jnp.float32
    shape = jax.ShapeDtypeStruct

    routes, weights = route_ids.T, gate_weights.T
    place = jnp.stack([lax.axis_index("core"), lax.axis_index("z_1")]).astype(jnp.int32)
    tokens, place = lax.optimization_barrier((tokens, place))

    swap = functools.partial(lax.ppermute, axis_name="core", perm=[(0, 1), (1, 0)])
    exchange = functools.partial(lax.all_to_all, split_axis=0, concat_axis=0, tiled=True)

    first_routes, first_tokens, up_rows = (
        pltpu.with_memory_space_constraint(v, pltpu.HBM) for v in (routes, tokens, w_up[0].T)
    )
    picked = call(
        dispatch_body,
        shape((experts, CAP, lanes), bf16),
        (HBM, HBM),
        [pltpu.VMEM(routes.shape, routes.dtype), pltpu.VMEM(tokens.shape, tokens.dtype), pltpu.SemaphoreType.DMA((2,))],
    )(first_routes, first_tokens)
    slices = exchange(picked, "expert").reshape(slots, lanes)
    scaled = call(scale_body, shape((slots + MARK_ROWS, lanes), bf16), (VMEM,))(slices)
    own = lax.all_gather(scaled.astype(jnp.float16), Z, axis=0, tiled=True)
    own = own.reshape(chips, *scaled.shape).astype(bf16)
    other = swap(own)

    of_parity = chips // PARITIES
    half = shape((experts, of_parity, CAP, lanes), bf16)
    quarter = shape((experts, of_parity // 2, CAP, lanes), bf16)
    wide = shape(half.shape, f32)
    acc = shape((slots, width), f32)
    held = shape((width, width_in), bf16)
    gate_rows, down_rows = w_gate[0].T, w_down[0]
    down_flops = slots * width * width_in // 2

    gate_half, up_half, up_here = call(
        first_half_body,
        (acc, acc, held),
        (SMEM, VMEM, VMEM, HBM),
        [pltpu.SemaphoreType.DMA((CHUNKS,))],
        flops=4 * down_flops,
    )(place, own, gate_rows, up_rows)
    hidden, theirs_away = call(
        second_half_body, (shape((slots, width), bf16), half), (SMEM,) + (VMEM,) * 6, flops=5 * down_flops
    )(place, other, gate_half, up_half, gate_rows, up_here, down_rows)
    arrived_away = swap(theirs_away)
    mine_away = call(
        functools.partial(down_body, own_core=True, own_parity=False), wide, (SMEM, VMEM, VMEM), flops=down_flops
    )(place, hidden, down_rows)
    right, left = call(outgoing_body, (quarter, quarter), (VMEM, VMEM))(mine_away, arrived_away)
    low = lax.ppermute(right, Z, [(z, (z + 1) % chips) for z in range(chips)])
    high = lax.ppermute(left, Z, [(z, (z - 1) % chips) for z in range(chips)])
    theirs = call(
        functools.partial(down_body, own_core=False, own_parity=True), half, (SMEM, VMEM, VMEM), flops=down_flops
    )(place, hidden, down_rows)
    arrived = swap(theirs)
    mine, combine_table = call(
        last_down_body, (wide, shape((token_count, slots), bf16)), (SMEM,) + (VMEM,) * 4, flops=down_flops
    )(place, hidden, down_rows, routes, weights)
    paired = call(pair_body, half, (VMEM,) * 4)(mine, arrived, low, high)

    results = exchange(paired, "expert")
    blended = call(combine_body, shape((of_parity, token_count, lanes), bf16), (VMEM, VMEM))(combine_table, results)
    pieces = exchange(blended, "z_0")
    return pieces.astype(f32).sum(axis=0).astype(bf16)


def solution(mesh):
    groups, experts, etp = (mesh.shape[name] for name in ("groups", "expert", "etp"))
    finer = Mesh(
        mesh.devices.reshape(groups, experts, etp // (CORES * PARITIES), PARITIES, CORES),
        ("groups", "expert", *ETP),
    )
    placed = (
        P(("groups", "expert"), ETP),
        P(("groups", "expert"), None),
        P(("groups", "expert"), None),
        P("expert", None, ETP),
        P("expert", None, ETP),
        P("expert", ETP, None),
    )
    return jax.shard_map(layer, mesh=finer, in_specs=placed, out_specs=P(("groups", "expert"), ETP), check_vma=False)
```
